128 devices in a mesh: tm: 2 (over core), space: 64 (over z, y, x).
Axes of the slice: x: 4, y: 4, z: 4, core: 2. Of those that a mesh axis runs over, the one named last changes fastest.
Arguments:
- fine: bfloat16 [8, 256, 256, 256], P('tm', 'space'), may hold values from -6 to 6
- coarse: bfloat16 [8, 128, 128, 256], P('tm', 'space'), may hold values from -6 to 6
- w_query: bfloat16 [256, 256], replicated, may hold values from -24 to 24
- w_key: bfloat16 [256, 256], replicated, may hold values from -0.375 to 0.375
- w_value: bfloat16 [256, 256], replicated, may hold values from -0.375 to 0.375
- w_out: bfloat16 [256, 256], replicated, may hold values from -0.375 to 0.375
- conv_first: bfloat16 [3, 3, 256, 256], replicated, may hold values from -0.125 to 0.125
- conv_second: bfloat16 [3, 3, 256, 256], replicated, may hold values from -0.125 to 0.125
Outputs:
- joined: bfloat16 [8, 256, 256, 256], P('tm', 'space')
The draws below stay inside these ranges and needn't reach their ends.
All inputs are finite; a program needn't handle non-finite values.
Results may differ from the reference program's by a relative error of at most 0.009.
Values may be sent and summed in bfloat16 or wider, within the bound.
No kernel may reach another device: no remote copies, remote signals or barrier semaphores. Data moves between devices by JAX's collectives and lax.ppermute only.
A program may use at most 128 MiB of HBM per device.

```python
import jax
import jax.numpy as jnp
from jax import lax

C = 256
HEADS = 8
W = 256
FRAMES = 8
H = 256


def draw_w_query(key, part):
    base = jax.random.normal(jax.random.fold_in(key, 11), (C, C), jnp.float32) / jnp.sqrt(jnp.float32(C))
    base = jnp.clip(base, -6.0 / jnp.sqrt(jnp.float32(C)), 6.0 / jnp.sqrt(jnp.float32(C)))
    logs = jax.random.uniform(jax.random.fold_in(key, 12), (HEADS,), jnp.float32, jnp.log(0.5), jnp.log(3.0))
    columns = jnp.repeat(jnp.exp(logs), C // HEADS)
    return (base * columns[None, :]).astype(jnp.bfloat16)


def shard_levels(own_key, extent, split, least, high):
    loudness, own = 1.0, jax.random.fold_in(own_key, 6)
    for axis_at, blocks in split:
        heights = jnp.exp(jax.random.uniform(jax.random.fold_in(own, axis_at), (blocks,), jnp.float32, least / len(split), high / len(split)))
        loudness = loudness * jnp.repeat(heights, extent[axis_at] // blocks).reshape([-1 if axis == axis_at else 1 for axis in range(len(extent))])
    return loudness


def scatter_about(own_key, extent, deviation, reach, shards=(), kind=jnp.bfloat16):
    entries = jax.random.normal(own_key, extent, jnp.float32) * deviation
    if len(shards) > 0:
        entries = shard_levels(own_key, extent, shards, -0.22, 0.18) * entries
    return jnp.clip(entries, min=-reach, max=reach).astype(kind)


def setup_inputs(seed: int = 0) -> dict:
    arg_keys = jax.random.split(jax.random.key(seed), 9)
    return {
        "fine": scatter_about(arg_keys[0], (FRAMES, H, W, C), 1.0, 6.0, ((0, 2), (1, 64))),
        "coarse": scatter_about(arg_keys[1], (FRAMES, H // 2, W // 2, C), 1.0, 6.0, ((0, 2), (1, 64))),
        "w_query": draw_w_query(jax.random.fold_in(arg_keys[8], 71), 0),
        "w_key": scatter_about(arg_keys[3], (C, C), C ** -0.5, 0.375),
        "w_value": scatter_about(arg_keys[4], (C, C), C ** -0.5, 0.375),
        "w_out": scatter_about(arg_keys[5], (C, C), C ** -0.5, 0.375),
        "conv_first": scatter_about(arg_keys[6], (3, 3, C, C), (9 * C) ** -0.5, 0.125),
        "conv_second": scatter_about(arg_keys[7], (3, 3, C, C), (9 * C) ** -0.5, 0.125),
    }


def encode(frame_ids, width):
    half = width // 2
    index = jnp.arange(half, dtype=jnp.float32)
    inverse = jnp.exp(-jnp.log(10000.0) * 2.0 * index / width)
    angles = frame_ids.astype(jnp.float32)[:, None] * inverse[None, :]
    return jnp.concatenate([jnp.sin(angles), jnp.cos(angles)], axis=1)

def normalize(features, frame_ids):
    width = features.shape[-1]
    hidden = features.astype(jnp.float32) + encode(frame_ids, width)[:, None, None, :]
    center = hidden - lax.optimization_barrier(jnp.mean(hidden, axis=-1, keepdims=True))
    spread = lax.optimization_barrier(jnp.mean(center * center, axis=-1, keepdims=True))
    return (center * lax.rsqrt(spread + 1e-05)).astype(jnp.bfloat16)

def project(normed, weight):
    shape = normed.shape
    flat = normed.reshape(-1, shape[-1])
    return jnp.dot(flat, weight, preferred_element_type=jnp.float32).astype(jnp.bfloat16).reshape(shape)

def attend(query, key, value):
    frames, rows, cols, width = query.shape
    depth = width // HEADS
    query_heads = query.reshape(frames, rows * cols, HEADS, depth).astype(jnp.float32)
    key_heads = key.reshape(key.shape[0], rows * cols, HEADS, depth).astype(jnp.float32)
    value_heads = value.reshape(value.shape[0], rows * cols, HEADS, depth).astype(jnp.float32)
    scores = jnp.einsum('qphd,kphd->qkhp', query_heads, key_heads) / jnp.sqrt(jnp.float32(depth))
    weights = jax.nn.softmax(scores, axis=1).astype(jnp.bfloat16)
    attended = jnp.einsum('qkhp,kphd->qphd', weights.astype(jnp.float32), value_heads)
    return attended.astype(jnp.bfloat16).reshape(frames, rows, cols, width)

def convolve(features, weight):
    return lax.conv_general_dilated(features.astype(jnp.float32), weight.astype(jnp.float32), (1, 1), 'SAME', dimension_numbers=('NHWC', 'HWIO', 'NHWC'), precision=lax.Precision.HIGHEST)

def double(extended, axis):
    count = extended.shape[axis] - 2
    middle = lax.slice_in_dim(extended, 1, count + 1, axis=axis)
    before = lax.slice_in_dim(extended, 0, count, axis=axis)
    after = lax.slice_in_dim(extended, 2, count + 2, axis=axis)
    even = 0.75 * middle + 0.25 * before
    odd = 0.75 * middle + 0.25 * after
    stacked = jnp.stack([even, odd], axis=axis + 1)
    shape = list(middle.shape)
    shape[axis] = 2 * count
    return stacked.reshape(shape)

def upsample(coarse):
    values = coarse.astype(jnp.float32)
    extended = jnp.pad(values, ((0, 0), (1, 1), (0, 0), (0, 0)), mode='edge')
    rows_done = double(extended, 1)
    extended = jnp.pad(rows_done, ((0, 0), (0, 0), (1, 1), (0, 0)), mode='edge')
    return double(extended, 2)

def reference(fine, coarse, w_query, w_key, w_value, w_out, conv_first, conv_second):
    frame_ids = jnp.arange(fine.shape[0], dtype=jnp.int32)
    normed = normalize(fine, frame_ids)
    query = project(normed, w_query)
    key = project(normed, w_key)
    value = project(normed, w_value)
    attended = attend(query, key, value)
    shape = fine.shape
    branch = jnp.dot(attended.reshape(-1, shape[-1]), w_out, preferred_element_type=jnp.float32).reshape(shape)
    moved = (fine.astype(jnp.float32) + branch).astype(jnp.bfloat16)
    first = convolve(jax.nn.relu(moved), conv_first).astype(jnp.bfloat16)
    second = convolve(jax.nn.relu(first), conv_second)
    up = upsample(coarse)
    return (up + moved.astype(jnp.float32) + second).astype(jnp.bfloat16)
```

```python
import jax
import jax.numpy as jnp
import numpy as np
from jax import lax
from jax.experimental import pallas as pl
from jax.experimental.pallas import tpu as pltpu
from jax.sharding import PartitionSpec as P

HEADS = 8
C = 256
D = C // HEADS
W = 256
F32 = jnp.float32
BF16 = jnp.bfloat16
VMEM_LIMIT = 56 * 1024 * 1024


def encode_table(frames, width):
    half = width // 2
    inverse = np.exp(-np.log(10000.0) * 2.0 * np.arange(half) / width)
    angles = np.arange(frames)[:, None] * inverse[None, :]
    table = np.concatenate([np.sin(angles), np.cos(angles)], axis=1)
    return table.astype(np.float32)


def dot(a, b):
    return jnp.dot(a, b, preferred_element_type=F32)


def attention_body(pos_ref, own_ref, other_ref, wq_ref, wk_ref, wv_ref, wo_ref,
                   moved_ref, up_ref, down_ref,
                   wqkv_s, wo_s, norm_s, q_s, k_s, v_s, att_s):
    row = pl.program_id(0)
    frames = own_ref.shape[0]

    @pl.when(row == 0)
    def _():
        to = lax.broadcasted_iota(jnp.int32, (C, C), 0)
        at = lax.broadcasted_iota(jnp.int32, (C, C), 1)
        pick = (at == (to % HEADS) * D + to // HEADS).astype(BF16)
        nt = (((1,), (1,)), ((), ()))
        for n, ref in enumerate((wq_ref, wk_ref, wv_ref)):
            wqkv_s[n * C:(n + 1) * C] = lax.dot_general(pick, ref[...], nt, preferred_element_type=F32).astype(BF16)
        wo_s[...] = dot(pick, wo_ref[...]).astype(BF16)

    for f in range(2 * frames):
        x_ref = own_ref if f < frames else other_ref
        i = f % frames
        for half in range(W // 128):
            lanes = slice(half * 128, half * 128 + 128)
            xt = x_ref[i, 0, lanes, :].T
            h = xt.astype(F32) + pos_ref[f]
            center = h - jnp.sum(h, axis=0, keepdims=True) * (1.0 / C)
            spread = jnp.sum(center * center, axis=0, keepdims=True) * (1.0 / C)
            norm_s[f % 2, :, lanes] = (center * lax.rsqrt(spread + 1e-05)).astype(BF16)
        if f < frames:
            y = dot(wqkv_s[...], norm_s[f % 2])
            q_s[i] = y[:C]
            k_s[f] = y[C:2 * C]
            v_s[f] = y[2 * C:]
        else:
            y = dot(wqkv_s[C:], norm_s[f % 2])
            k_s[f] = y[:C]
            v_s[f] = y[C:]

    factor = float(np.log2(np.e) / np.sqrt(D))
    keys = 2 * frames
    for half in range(W // 128):
        lanes = slice(half * 128, half * 128 + 128)

        def score(d, acc):
            at = pl.ds(pl.multiple_of(d * HEADS, HEADS), HEADS)
            qs = [q_s[a, at, lanes] for a in range(frames)]
            ks = [k_s[b, at, lanes] for b in range(keys)]
            return tuple(acc[a * keys + b] + qs[a] * ks[b] for a in range(frames) for b in range(keys))

        zero = jnp.zeros((HEADS, 128), F32)
        acc = lax.fori_loop(0, D, score, (zero,) * (frames * keys), unroll=4)
        weights = []
        for a in range(frames):
            line = acc[a * keys:(a + 1) * keys]
            top = line[0]
            for s in line[1:]:
                top = jnp.maximum(top, s)
            powers = [jnp.exp2((s - top) * factor) for s in line]
            total = powers[0]
            for p in powers[1:]:
                total = total + p
            inv = 1.0 / total
            weights += [p * inv for p in powers]

        def gather(d2, _):
            outs = [[] for _ in range(frames)]
            for sub in range(2):
                at = pl.ds(pl.multiple_of(d2 * 2 * HEADS + sub * HEADS, HEADS), HEADS)
                vs = [v_s[b, at, lanes] for b in range(keys)]
                for a in range(frames):
                    total = weights[a * keys] * vs[0]
                    for b in range(1, keys):
                        total = total + weights[a * keys + b] * vs[b]
                    outs[a].append(total)
            at = pl.ds(pl.multiple_of(d2 * 2 * HEADS, 2 * HEADS), 2 * HEADS)
            for a in range(frames):
                att_s[a, at, lanes] = jnp.concatenate(outs[a], axis=0).astype(BF16)
            return 0

        lax.fori_loop(0, D // 2, gather, 0, unroll=2)

    for a in range(frames):
        branch = lax.dot_general(att_s[a], wo_s[...], (((0,), (0,)), ((), ())), preferred_element_type=F32)
        moved = (own_ref[a, 0].astype(F32) + branch).astype(BF16)
        moved_ref[a, 0] = moved
        up_ref[a, 0] = moved

        @pl.when(row <= 1)
        def _():
            down_ref[a, 0] = moved


def attention(pos, own, other, w_query, w_key, w_value, w_out):
    frames, rows = own.shape[:2]
    block = (frames, 1, W, C)
    by_row = pl.BlockSpec(block, lambda r: (0, r, 0, 0))
    whole = pl.BlockSpec((C, C), lambda r: (0, 0))
    return pl.pallas_call(
        attention_body,
        grid=(rows,),
        in_specs=[pl.BlockSpec(pos.shape, lambda r: (0, 0, 0)), by_row, by_row, whole, whole, whole, whole],
        out_specs=[by_row,
                   pl.BlockSpec(block, lambda r: (0, jnp.maximum(r - (rows - 2), 0), 0, 0)),
                   pl.BlockSpec(block, lambda r: (0, jnp.minimum(r, 1), 0, 0))],
        out_shape=[jax.ShapeDtypeStruct(own.shape, BF16),
                   jax.ShapeDtypeStruct((frames, 2, W, C), BF16),
                   jax.ShapeDtypeStruct((frames, 2, W, C), BF16)],
        scratch_shapes=[pltpu.VMEM((3 * C, C), BF16), pltpu.VMEM((C, C), BF16),
                        pltpu.VMEM((2, C, W), BF16),
                        pltpu.VMEM((frames, C, W), F32), pltpu.VMEM((2 * frames, C, W), F32),
                        pltpu.VMEM((2 * frames, C, W), F32), pltpu.VMEM((frames, C, W), BF16)],
        compiler_params=pltpu.CompilerParams(dimension_semantics=("arbitrary",), vmem_limit_bytes=VMEM_LIMIT),
        name="attention",
    )(pos, own, other, w_query, w_key, w_value, w_out)


def shifted(value, pad_s, out, at):
    pad_s[8:8 + W] = value.astype(F32)
    out[1, at] = value
    out[0, at] = pad_s[7:7 + W].astype(BF16)
    out[2, at] = pad_s[9:9 + W].astype(BF16)


def conv_body(edge_ref, moved_ref, above_ref, below_ref, coarse_ref, ca_ref, cb_ref, w1_ref, w2_ref,
              out_ref, pad_s, in_s, mid_s, coarse_s, lift_s):
    rows = moved_ref.shape[1]
    first_edge = edge_ref[0] == 1
    last_edge = edge_ref[1] == 1

    @pl.when(pl.program_id(0) == 0)
    def _():
        pad_s[0:8] = jnp.zeros((8, C), F32)
        pad_s[8 + W:16 + W] = jnp.zeros((8, C), F32)
        x = lax.broadcasted_iota(jnp.int32, (W, W), 0)
        at = lax.broadcasted_iota(jnp.int32, (W, W), 1)
        high = at // (W // 2)
        col = at % (W // 2)
        near = x // 2
        far = jnp.clip(near + 2 * (x % 2) - 1, 0, W // 2 - 1)
        base = 0.75 * (col == near).astype(F32) + 0.25 * (col == far).astype(F32)
        lift_s[0] = (base * jnp.where(high == 1, 0.75, 0.25)).astype(BF16)
        lift_s[1] = (base * jnp.where(high == 1, 0.25, 0.75)).astype(BF16)

    half = W // 2
    coarse_rows = rows // 2
    top = coarse_ref[0, 0]
    bottom = coarse_ref[0, coarse_rows - 1]
    coarse_s[0:half] = jnp.where(first_edge, top, ca_ref[0, 0])
    for r in range(coarse_rows):
        coarse_s[half * (r + 1):half * (r + 2)] = coarse_ref[0, r]
    coarse_s[half * (coarse_rows + 1):half * (coarse_rows + 2)] = jnp.where(last_edge, bottom, cb_ref[0, 0])

    zero = jnp.zeros((), BF16)
    for r in range(rows + 4):
        if r < 2:
            value = above_ref[0, r]
        elif r < rows + 2:
            value = moved_ref[0, r - 2]
        else:
            value = below_ref[0, r - rows - 2]
        shifted(jnp.maximum(value, zero), pad_s, in_s, slice(r * W, (r + 1) * W))

    def first(j, _):
        start = pl.multiple_of(j * W, W)
        total = None
        for dy in range(3):
            for dx in range(3):
                part = dot(in_s[dx, pl.ds(start + dy * W, W)], w1_ref[dy, dx])
                total = part if total is None else total + part
        value = jnp.maximum(total, 0.0).astype(BF16)
        outside = jnp.logical_or(jnp.logical_and(first_edge, j == 0), jnp.logical_and(last_edge, j == rows + 1))
        value = jnp.where(outside, jnp.zeros_like(value), value)
        shifted(value, pad_s, mid_s, pl.ds(start, W))
        return 0

    lax.fori_loop(0, rows + 2, first, 0)

    for j in range(rows):
        total = dot(lift_s[j % 2], coarse_s[((j + 1) // 2) * half:((j + 1) // 2) * half + W])
        for dy in range(3):
            for dx in range(3):
                total = total + dot(mid_s[dx, (j + dy) * W:(j + dy + 1) * W], w2_ref[dy, dx])
        out_ref[0, j] = (total + moved_ref[0, j].astype(F32)).astype(BF16)


def convolutions(edge, moved, above, below, coarse, ca, cb, conv_first, conv_second):
    frames, rows = moved.shape[:2]
    coarse_rows = coarse.shape[1]

    def by_frame(n, w):
        return pl.BlockSpec((1, n, w, C), lambda f: (f, 0, 0, 0))

    whole = pl.BlockSpec(conv_first.shape, lambda f: (0, 0, 0, 0))
    return pl.pallas_call(
        conv_body,
        grid=(frames,),
        in_specs=[pl.BlockSpec(memory_space=pltpu.SMEM), by_frame(rows, W), by_frame(2, W), by_frame(2, W),
                  by_frame(coarse_rows, W // 2), by_frame(1, W // 2), by_frame(1, W // 2), whole, whole],
        out_specs=by_frame(rows, W),
        out_shape=jax.ShapeDtypeStruct(moved.shape, BF16),
        scratch_shapes=[pltpu.VMEM((W + 16, C), F32), pltpu.VMEM((3, (rows + 4) * W, C), BF16),
                        pltpu.VMEM((3, (rows + 2) * W, C), BF16),
                        pltpu.VMEM(((coarse_rows + 2) * W // 2, C), BF16), pltpu.VMEM((2, W, W), BF16)],
        compiler_params=pltpu.CompilerParams(dimension_semantics=("arbitrary",), vmem_limit_bytes=VMEM_LIMIT),
        name="convolutions",
    )(edge, moved, above, below, coarse, ca, cb, conv_first, conv_second)


def local(fine, coarse, w_query, w_key, w_value, w_out, conv_first, conv_second):
    frames = fine.shape[0]
    tm = lax.axis_index("tm")
    size = lax.axis_size("space")
    here = lax.axis_index("space")
    up = [(i, i + 1) for i in range(size - 1)]
    down = [(i + 1, i) for i in range(size - 1)]
    other = lax.ppermute(fine, "tm", [(0, 1), (1, 0)])
    ca = lax.ppermute(coarse[:, -1:], "space", up)
    cb = lax.ppermute(coarse[:, :1], "space", down)
    table = jnp.broadcast_to(jnp.asarray(encode_table(2 * frames, C))[:, :, None], (2 * frames, C, 128))
    pos = jnp.where(tm == 0, table, jnp.roll(table, frames, axis=0))
    moved, up_rows, down_rows = attention(pos, fine, other, w_query, w_key, w_value, w_out)
    above = lax.ppermute(up_rows, "space", up)
    below = lax.ppermute(down_rows, "space", down)
    edge = jnp.stack([here == 0, here == size - 1]).astype(jnp.int32)
    return convolutions(edge, moved, above, below, coarse, ca, cb, conv_first, conv_second)


def solution(mesh):
    split = P("tm", "space", None, None)
    return jax.shard_map(
        local,
        mesh=mesh,
        in_specs=(split, split, P(), P(), P(), P(), P(), P()),
        out_specs=split,
        check_vma=False,
    )
```

```python
import jax
import jax.numpy as jnp
import numpy as np
from jax import lax
from jax.experimental import pallas as pl
from jax.experimental.pallas import tpu as pltpu
from jax.sharding import PartitionSpec as P

HEADS = 8
C = 256
D = C // HEADS
W = 256
HALF = W // 2
F32 = jnp.float32
BF16 = jnp.bfloat16
VMEM_LIMIT = 20 * 1024 * 1024


def encode_table(frames, width):
    half = width // 2
    inverse = np.exp(-np.log(10000.0) * 2.0 * np.arange(half) / width)
    angles = np.arange(frames)[:, None] * inverse[None, :]
    table = np.concatenate([np.sin(angles), np.cos(angles)], axis=1).astype(np.float32)
    return np.ascontiguousarray(np.broadcast_to(table[:, :, None], (frames, width, 128)))


def dot(a, b):
    return jnp.dot(a, b, preferred_element_type=F32)


def normed_row(x_ref, i, row, pos, norm):
    for half in range(W // 128):
        lanes = slice(half * 128, half * 128 + 128)
        h = x_ref[i, row, lanes, :].T.astype(F32) + pos
        center = h - jnp.sum(h, axis=0, keepdims=True) * (1.0 / C)
        spread = jnp.sum(center * center, axis=0, keepdims=True) * (1.0 / C)
        norm[:, lanes] = (center * lax.rsqrt(spread + 1e-05)).astype(BF16)


def attention_row(row, pos_ref, own_ref, other_ref, wkv_ref, wo_ref, q_ref, ko_ref, vo_ref, out_ref,
                  norm_s, k_s, v_s, att_s):
    frames = own_ref.shape[0]
    keys = 2 * frames
    base = (1 - lax.axis_index("tm")) * frames

    for f in range(frames):
        normed_row(other_ref, f, row, pos_ref[base + f], norm_s.at[f])
        y = dot(wkv_ref[C:], norm_s[f])
        k_s[f] = y[:C]
        v_s[f] = y[C:]

    factor = float(np.log2(np.e) / np.sqrt(D))
    for half in range(W // 128):
        lanes = slice(half * 128, half * 128 + 128)

        def score(d, acc):
            at = pl.ds(pl.multiple_of(d * HEADS, HEADS), HEADS)
            qs = [q_ref[row, a, at, lanes] for a in range(frames)]
            ks = [ko_ref[row, b, at, lanes] for b in range(frames)] + [k_s[b, at, lanes] for b in range(frames)]
            return tuple(acc[a * keys + b] + qs[a] * ks[b] for a in range(frames) for b in range(keys))

        zero = jnp.zeros((HEADS, 128), F32)
        acc = lax.fori_loop(0, D, score, (zero,) * (frames * keys), unroll=4)
        weights = []
        for a in range(frames):
            line = acc[a * keys:(a + 1) * keys]
            top = line[0]
            for s in line[1:]:
                top = jnp.maximum(top, s)
            powers = [jnp.exp2((s - top) * factor) for s in line]
            total = powers[0]
            for p in powers[1:]:
                total = total + p
            inv = 1.0 / total
            weights += [p * inv for p in powers]

        def gather(d2, _):
            outs = [[] for _ in range(frames)]
            for sub in range(2):
                at = pl.ds(pl.multiple_of(d2 * 2 * HEADS + sub * HEADS, HEADS), HEADS)
                vs = [vo_ref[row, b, at, lanes] for b in range(frames)] + [v_s[b, at, lanes] for b in range(frames)]
                for a in range(frames):
                    total = weights[a * keys] * vs[0]
                    for b in range(1, keys):
                        total = total + weights[a * keys + b] * vs[b]
                    outs[a].append(total)
            at = pl.ds(pl.multiple_of(d2 * 2 * HEADS, 2 * HEADS), 2 * HEADS)
            for a in range(frames):
                att_s[a, at, lanes] = jnp.concatenate(outs[a], axis=0).astype(BF16)
            return 0

        lax.fori_loop(0, D // 2, gather, 0, unroll=2)

    for a in range(frames):
        branch = lax.dot_general(att_s[a], wo_ref[...], (((0,), (0,)), ((), ())), preferred_element_type=F32)
        out_ref[a, :W] = (own_ref[a, row].astype(F32) + branch).astype(BF16)


def own_body(pos_hbm, own_hbm, wq_hbm, wk_hbm, wv_hbm, wo_hbm,
             pos_ref, own_ref, wqkv_ref, wor_ref, q_ref, k_ref, v_ref, w_s, norm_s, sems):
    frames, rows = own_hbm.shape[:2]
    loads = [pltpu.make_async_copy(ref, w_s.at[n], sems.at[n]) for n, ref in enumerate((wq_hbm, wk_hbm, wv_hbm, wo_hbm))]
    loads.append(pltpu.make_async_copy(pos_hbm, pos_ref, sems.at[4]))
    loads.append(pltpu.make_async_copy(own_hbm, own_ref, sems.at[5]))
    for load in loads:
        load.start()
    to = lax.broadcasted_iota(jnp.int32, (C, C), 0)
    at = lax.broadcasted_iota(jnp.int32, (C, C), 1)
    pick = (at == (to % HEADS) * D + to // HEADS).astype(BF16)
    nt = (((1,), (1,)), ((), ()))
    for load in loads[:4]:
        load.wait()
    for n in range(3):
        wqkv_ref[n * C:(n + 1) * C] = lax.dot_general(pick, w_s[n], nt, preferred_element_type=F32).astype(BF16)
    wor_ref[...] = dot(pick, w_s[3]).astype(BF16)
    for load in loads[4:]:
        load.wait()
    base = lax.axis_index("tm") * frames

    def one(row, _):
        for f in range(frames):
            normed_row(own_ref, f, row, pos_ref[base + f], norm_s.at[f])
            y = dot(wqkv_ref[...], norm_s[f])
            q_ref[row, f] = y[:C]
            k_ref[row, f] = y[C:2 * C]
            v_ref[row, f] = y[2 * C:]
        return 0

    lax.fori_loop(0, rows, one, 0)


def outer_body(pos_ref, own_ref, other_ref, wqkv_ref, wo_ref, q_ref, k_ref, v_ref, coarse_ref, down_ref, up_ref,
               *scratch):
    for n, (row, ref) in enumerate(((0, down_ref), (own_ref.shape[1] - 1, up_ref))):
        attention_row(row, pos_ref, own_ref, other_ref, wqkv_ref, wo_ref, q_ref, k_ref, v_ref, ref, *scratch)
        ref[:, W:] = coarse_ref[:, n * (coarse_ref.shape[1] - 1)]


def inner_body(pos_ref, own_ref, other_ref, wqkv_ref, wo_ref, q_ref, k_ref, v_ref, down_ref, up_ref, *scratch):
    for row, ref in ((1, down_ref), (own_ref.shape[1] - 2, up_ref)):
        attention_row(row, pos_ref, own_ref, other_ref, wqkv_ref, wo_ref, q_ref, k_ref, v_ref, ref, *scratch)


def call(body, name, args, outs, scratch, space=pltpu.VMEM):
    return pl.pallas_call(
        body,
        in_specs=[pl.BlockSpec(memory_space=space)] * len(args),
        out_specs=[pl.BlockSpec(memory_space=pltpu.VMEM)] * len(outs),
        out_shape=[jax.ShapeDtypeStruct(s, t) for s, t in outs],
        scratch_shapes=scratch,
        compiler_params=pltpu.CompilerParams(vmem_limit_bytes=VMEM_LIMIT),
        name=name,
    )(*args)


def own_projections(pos, own, *weights):
    frames, rows = own.shape[:2]
    wide = ((rows, frames, C, W), F32)
    args = [pltpu.with_memory_space_constraint(a, pltpu.HBM) for a in (pos, own, *weights)]
    return call(own_body, "own_projections", args,
                [(pos.shape, F32), (own.shape, BF16), ((3 * C, C), BF16), ((C, C), BF16), wide, wide, wide],
                [pltpu.VMEM((4, C, C), BF16), pltpu.VMEM((frames, C, W), BF16), pltpu.SemaphoreType.DMA((6,))], pltpu.HBM)


def attention(coarse, *args):
    frames = args[1].shape[0]
    if coarse is None:
        body, width, name = inner_body, W, "attention_inner"
    else:
        body, width, name = outer_body, W + HALF, "attention_outer"
        args = args + (coarse,)
    return call(body, name, args, [((frames, width, C), BF16)] * 2,
                [pltpu.VMEM((frames, C, W), BF16), pltpu.VMEM((frames, C, W), F32),
                 pltpu.VMEM((frames, C, W), F32), pltpu.VMEM((frames, C, W), BF16)])


def clear_pads(pad_s):
    for r in range(pad_s.shape[0]):
        pad_s[r, 0:8] = jnp.zeros((8, C), F32)
        pad_s[r, 8 + W:16 + W] = jnp.zeros((8, C), F32)


def shifted(value, pad, out_s, row):
    pad[8:8 + W] = value.astype(F32)
    at = slice(row * W, (row + 1) * W)
    out_s[1, at] = value
    out_s[0, at] = pad[7:7 + W].astype(BF16)
    out_s[2, at] = pad[9:9 + W].astype(BF16)


def taps(source_s, row, w_ref, total=None, steps=(0, 1, 2)):
    for n, dy in enumerate(steps):
        for dx in range(3):
            part = dot(source_s[dx, (row + n) * W:(row + n + 1) * W], w_ref[dy, dx])
            total = part if total is None else total + part
    return total


def relu(value):
    return jnp.maximum(value, jnp.zeros((), value.dtype))


def lift_matrix(flip):
    x = lax.broadcasted_iota(jnp.int32, (W, W), 0)
    at = lax.broadcasted_iota(jnp.int32, (W, W), 1)
    high = at // HALF
    col = at % HALF
    near = x // 2
    far = jnp.clip(near + 2 * (x % 2) - 1, 0, HALF - 1)
    base = 0.75 * (col == near).astype(F32) + 0.25 * (col == far).astype(F32)
    return (base * jnp.where(high == flip, 0.25, 0.75)).astype(BF16)


def stage_one(m0_ref, m1_ref, m2_ref, m3_ref, w1_ref, mid_ref, pad_s, in_s):
    clear_pads(pad_s)

    def frame(f, _):
        for r, ref in enumerate((m0_ref, m1_ref, m2_ref, m3_ref)):
            shifted(relu(ref[f, :W]), pad_s.at[r], in_s, r)
        for j in range(2):
            mid_ref[f, j] = relu(taps(in_s, j, w1_ref)).astype(BF16)
        return 0

    lax.fori_loop(0, m0_ref.shape[0], frame, 0)


def stage_two(above_ref, m0_ref, m1_ref, m2_ref, m3_ref, below_ref, mid_ref, coarse_ref, w1_ref, w2_ref,
              inner_ref, first_ref, second_ref, pad_s, in_s, mid_s, lift_s, coarse_s):
    here = lax.axis_index("space")
    first_edge = here == 0
    last_edge = here == lax.axis_size("space") - 1
    clear_pads(pad_s)
    lift_s[0] = lift_matrix(0)
    lift_s[1] = lift_matrix(1)

    def frame(f, _):
        near, far = coarse_ref[f, 0], coarse_ref[f, 1]
        coarse_s[0:HALF] = jnp.where(first_edge, near, above_ref[f, W:])
        coarse_s[HALF:2 * HALF] = near
        coarse_s[2 * HALF:3 * HALF] = far
        coarse_s[3 * HALF:] = jnp.where(last_edge, far, below_ref[f, W:])
        for r, ref in enumerate((above_ref, m0_ref, m1_ref, m2_ref, m3_ref, below_ref)):
            shifted(relu(ref[f, :W]), pad_s.at[r], in_s, r)
        for j in range(2):
            shifted(mid_ref[f, j], pad_s.at[6 + j], mid_s, j + 1)
        for j in range(2):
            shifted(relu(taps(in_s, 3 * j, w1_ref)).astype(BF16), pad_s.at[8 + j], mid_s, 3 * j)
        for j, steps in enumerate(((1, 2), (0, 1))):
            first_ref[f, j] = taps(in_s, 4 * j, w1_ref, None, steps)
        for j, ref in enumerate((m1_ref, m2_ref)):
            total = taps(mid_s, j, w2_ref, dot(lift_s[1 - j], coarse_s[HALF:3 * HALF]))
            inner_ref[f, j] = (total + ref[f].astype(F32)).astype(BF16)
        for j, (ref, steps) in enumerate(((m0_ref, (1, 2)), (m3_ref, (0, 1)))):
            total = taps(mid_s, 2 * j, w2_ref, dot(lift_s[j], coarse_s[2 * j * HALF:(2 * j + 2) * HALF]), steps)
            second_ref[f, j] = total + ref[f, :W].astype(F32)
        return 0

    lax.fori_loop(0, m0_ref.shape[0], frame, 0)


def stage_three(above_ref, below_ref, inner_ref, first_ref, second_ref, w1_ref, w2_ref, out_ref, pad_s, in_s, mid_s):
    here = lax.axis_index("space")
    edges = (here == 0, here == lax.axis_size("space") - 1)
    clear_pads(pad_s)
    frames = above_ref.shape[0]
    for f in range(frames):
        for j, (ref, edge) in enumerate(zip((above_ref, below_ref), edges)):
            n = 2 * f + j
            step = (2 * j,)
            shifted(relu(ref[f]), pad_s.at[n], in_s, n)
            value = relu(taps(in_s, n, w1_ref, first_ref[f, j], step)).astype(BF16)
            value = jnp.where(edge, jnp.zeros_like(value), value)
            shifted(value, pad_s.at[2 * frames + n], mid_s, n)
            out_ref[f, 3 * j] = taps(mid_s, n, w2_ref, second_ref[f, j], step).astype(BF16)
            out_ref[f, 1 + j] = inner_ref[f, j]


def planes(rows):
    return pltpu.VMEM((3, rows * W, C), BF16)


def pads(rows):
    return pltpu.VMEM((rows, W + 16, C), F32)


def local(fine, coarse, w_query, w_key, w_value, w_out, conv_first, conv_second):
    frames = fine.shape[0]
    size = lax.axis_size("space")
    up = [(i, i + 1) for i in range(size - 1)]
    down = [(i + 1, i) for i in range(size - 1)]
    other = lax.ppermute(fine, "tm", [(0, 1), (1, 0)])
    pos = jnp.asarray(encode_table(2 * frames, C))
    ready = own_projections(pos, fine, w_query, w_key, w_value, w_out)
    held_pos, held, *ready = ready
    m0, m3 = attention(coarse, held_pos, held, other, *ready)
    above = lax.ppermute(m3, "space", up)
    below = lax.ppermute(m0, "space", down)
    m1, m2 = attention(None, held_pos, held, other, *ready)
    above2 = lax.ppermute(m2, "space", up)
    below2 = lax.ppermute(m1, "space", down)
    pair = (frames, 2, W, C)
    (mid,) = call(stage_one, "stage_one", (m0, m1, m2, m3, conv_first), [(pair, BF16)], [pads(4), planes(4)])
    inner, first, second = call(
        stage_two, "stage_two", (above, m0, m1, m2, m3, below, mid, coarse, conv_first, conv_second),
        [(pair, BF16), (pair, F32), (pair, F32)],
        [pads(10), planes(6), planes(4), pltpu.VMEM((2, W, W), BF16), pltpu.VMEM((4 * HALF, C), BF16)])
    (out,) = call(stage_three, "stage_three", (above2, below2, inner, first, second, conv_first, conv_second),
                  [((frames, 4, W, C), BF16)], [pads(4 * frames), planes(2 * frames), planes(2 * frames)])
    return out


def solution(mesh):
    split = P("tm", "space", None, None)
    return jax.shard_map(
        local,
        mesh=mesh,
        in_specs=(split, split, P(), P(), P(), P(), P(), P()),
        out_specs=split,
        check_vma=False,
    )
```

```python
import functools

import jax
import jax.numpy as jnp
import numpy as np
from jax import lax
from jax.experimental import pallas as pl
from jax.experimental.pallas import tpu as pltpu
from jax.sharding import PartitionSpec as P

HEADS = 8
C = 256
D = C // HEADS
W = 256
HALF = W // 2
F32 = jnp.float32
BF16 = jnp.bfloat16
VMEM_LIMIT = 20 * 1024 * 1024


def encode_table(frames, width):
    half = width // 2
    inverse = np.exp(-np.log(10000.0) * 2.0 * np.arange(half) / width)
    angles = np.arange(frames)[:, None] * inverse[None, :]
    table = np.concatenate([np.sin(angles), np.cos(angles)], axis=1).astype(np.float32)
    return np.ascontiguousarray(np.broadcast_to(table[:, :, None], (frames, width, 128)))


def dot(a, b):
    return jnp.dot(a, b, preferred_element_type=F32)


def normed_row(x_ref, i, row, pos, norm):
    for half in range(W // 128):
        lanes = slice(half * 128, half * 128 + 128)
        h = x_ref[i, row, lanes, :].T.astype(F32) + pos
        center = h - jnp.sum(h, axis=0, keepdims=True) * (1.0 / C)
        spread = jnp.sum(center * center, axis=0, keepdims=True) * (1.0 / C)
        norm[:, lanes] = (center * lax.rsqrt(spread + 1e-05)).astype(BF16)


def own_row(at_row, row, pos_ref, own_ref, wqkv_ref, q_ref, k_ref, v_ref, norm_s):
    frames = own_ref.shape[0]
    base = lax.axis_index("tm") * frames
    for f in range(frames):
        normed_row(own_ref, f, row, pos_ref[base + f], norm_s.at[f])
        y = dot(wqkv_ref[...], norm_s[f])
        q_ref[at_row, f] = y[:C]
        k_ref[at_row, f] = y[C:2 * C]
        v_ref[at_row, f] = y[2 * C:]


def attention_row(at_row, row, pos_ref, own_ref, other_ref, wkv_ref, wo_ref, q_ref, ko_ref, vo_ref, out_ref,
                  norm_s, k_s, v_s, att_s):
    frames = own_ref.shape[0]
    keys = 2 * frames
    base = (1 - lax.axis_index("tm")) * frames

    for f in range(frames):
        normed_row(other_ref, f, row, pos_ref[base + f], norm_s.at[f])
        y = dot(wkv_ref[C:], norm_s[f])
        k_s[f] = y[:C]
        v_s[f] = y[C:]

    factor = float(np.log2(np.e) / np.sqrt(D))
    for half in range(W // 128):
        lanes = slice(half * 128, half * 128 + 128)

        def score(d, acc):
            at = pl.ds(pl.multiple_of(d * HEADS, HEADS), HEADS)
            qs = [q_ref[at_row, a, at, lanes] for a in range(frames)]
            ks = [ko_ref[at_row, b, at, lanes] for b in range(frames)] + [k_s[b, at, lanes] for b in range(frames)]
            return tuple(acc[a * keys + b] + qs[a] * ks[b] for a in range(frames) for b in range(keys))

        zero = jnp.zeros((HEADS, 128), F32)
        acc = lax.fori_loop(0, D, score, (zero,) * (frames * keys), unroll=4)
        weights = []
        for a in range(frames):
            line = acc[a * keys:(a + 1) * keys]
            top = line[0]
            for s in line[1:]:
                top = jnp.maximum(top, s)
            powers = [jnp.exp2((s - top) * factor) for s in line]
            total = powers[0]
            for p in powers[1:]:
                total = total + p
            inv = 1.0 / total
            weights += [p * inv for p in powers]

        def gather(d2, _):
            outs = [[] for _ in range(frames)]
            for sub in range(2):
                at = pl.ds(pl.multiple_of(d2 * 2 * HEADS + sub * HEADS, HEADS), HEADS)
                vs = [vo_ref[at_row, b, at, lanes] for b in range(frames)] + [v_s[b, at, lanes] for b in range(frames)]
                for a in range(frames):
                    total = weights[a * keys] * vs[0]
                    for b in range(1, keys):
                        total = total + weights[a * keys + b] * vs[b]
                    outs[a].append(total)
            at = pl.ds(pl.multiple_of(d2 * 2 * HEADS, 2 * HEADS), 2 * HEADS)
            for a in range(frames):
                att_s[a, at, lanes] = jnp.concatenate(outs[a], axis=0).astype(BF16)
            return 0

        lax.fori_loop(0, D // 2, gather, 0, unroll=2)

    for a in range(frames):
        branch = lax.dot_general(att_s[a], wo_ref[...], (((0,), (0,)), ((), ())), preferred_element_type=F32)
        out_ref[a, :W] = (own_ref[a, row].astype(F32) + branch).astype(BF16)


def own_body(pos_hbm, own_hbm, wq_hbm, wk_hbm, wv_hbm, wo_hbm,
             pos_ref, own_ref, wqkv_ref, wor_ref, q_ref, k_ref, v_ref, w_s, norm_s, sems):
    frames, rows = own_hbm.shape[:2]
    loads = [pltpu.make_async_copy(ref, w_s.at[n], sems.at[n]) for n, ref in enumerate((wq_hbm, wk_hbm, wv_hbm, wo_hbm))]
    loads.append(pltpu.make_async_copy(pos_hbm, pos_ref, sems.at[4]))
    loads.append(pltpu.make_async_copy(own_hbm, own_ref, sems.at[5]))
    for load in loads:
        load.start()
    to = lax.broadcasted_iota(jnp.int32, (C, C), 0)
    at = lax.broadcasted_iota(jnp.int32, (C, C), 1)
    pick = (at == (to % HEADS) * D + to // HEADS).astype(BF16)
    nt = (((1,), (1,)), ((), ()))
    for load in loads[:4]:
        load.wait()
    for n in range(3):
        wqkv_ref[n * C:(n + 1) * C] = lax.dot_general(pick, w_s[n], nt, preferred_element_type=F32).astype(BF16)
    wor_ref[...] = dot(pick, w_s[3]).astype(BF16)
    for load in loads[4:]:
        load.wait()
    for n, row in enumerate((0, own_ref.shape[1] - 1)):
        own_row(n, row, pos_ref, own_ref, wqkv_ref, q_ref, k_ref, v_ref, norm_s)


def outer_body(pos_ref, own_ref, other_ref, wqkv_ref, wo_ref, q_ref, k_ref, v_ref, coarse_ref, down_ref, up_ref,
               norm_s, k_s, v_s, att_s):
    for n, (row, ref) in enumerate(((0, down_ref), (own_ref.shape[1] - 1, up_ref))):
        attention_row(n, row, pos_ref, own_ref, other_ref, wqkv_ref, wo_ref, q_ref, k_ref, v_ref, ref,
                      norm_s, k_s, v_s, att_s)
        ref[:, W:] = coarse_ref[:, n * (coarse_ref.shape[1] - 1)]


def inner_body(pos_ref, own_ref, other_ref, wqkv_ref, wo_ref, before_ref, down_ref, up_ref,
               norm_s, k_s, v_s, att_s, q_s, ko_s, vo_s):
    del before_ref
    for row, ref in ((1, down_ref), (own_ref.shape[1] - 2, up_ref)):
        own_row(0, row, pos_ref, own_ref, wqkv_ref, q_s, ko_s, vo_s, norm_s)
        attention_row(0, row, pos_ref, own_ref, other_ref, wqkv_ref, wo_ref, q_s, ko_s, vo_s, ref,
                      norm_s, k_s, v_s, att_s)


def call(body, name, args, outs, scratch, micros, space=pltpu.VMEM):
    return pl.pallas_call(
        body,
        in_specs=[pl.BlockSpec(memory_space=space)] * len(args),
        out_specs=[pl.BlockSpec(memory_space=pltpu.VMEM)] * len(outs),
        out_shape=[jax.ShapeDtypeStruct(s, t) for s, t in outs],
        scratch_shapes=scratch,
        compiler_params=pltpu.CompilerParams(vmem_limit_bytes=VMEM_LIMIT),
        cost_estimate=pl.CostEstimate(flops=micros * 10**9, transcendentals=0, bytes_accessed=1 << 20),
        name=name,
    )(*args)


def own_projections(pos, own, *weights):
    frames, rows = own.shape[:2]
    wide = ((2, frames, C, W), F32)
    args = [pltpu.with_memory_space_constraint(a, pltpu.HBM) for a in (pos, own, *weights)]
    return call(own_body, "own_projections", args,
                [(pos.shape, F32), (own.shape, BF16), ((3 * C, C), BF16), ((C, C), BF16), wide, wide, wide],
                [pltpu.VMEM((4, C, C), BF16), pltpu.VMEM((frames, C, W), BF16), pltpu.SemaphoreType.DMA((6,))], 6, pltpu.HBM)


def attention(body, name, args, width, extra, micros):
    frames = args[1].shape[0]
    return call(body, name, args, [((frames, width, C), BF16)] * 2,
                [pltpu.VMEM((frames, C, W), BF16), pltpu.VMEM((frames, C, W), F32),
                 pltpu.VMEM((frames, C, W), F32), pltpu.VMEM((frames, C, W), BF16)] + extra, micros)


def clear_pads(pad_s):
    for r in range(pad_s.shape[0]):
        pad_s[r, 0:8] = jnp.zeros((8, C), F32)
        pad_s[r, 8 + W:16 + W] = jnp.zeros((8, C), F32)


def shifted(value, pad, out_s, row):
    pad[8:8 + W] = value.astype(F32)
    at = slice(row * W, (row + 1) * W)
    out_s[1, at] = value
    out_s[0, at] = pad[7:7 + W].astype(BF16)
    out_s[2, at] = pad[9:9 + W].astype(BF16)


def taps(source_s, row, w_ref, total=None, steps=(0, 1, 2)):
    for n, dy in enumerate(steps):
        for dx in range(3):
            part = dot(source_s[dx, (row + n) * W:(row + n + 1) * W], w_ref[dy, dx])
            total = part if total is None else total + part
    return total


def relu(value):
    return jnp.maximum(value, jnp.zeros((), value.dtype))


def lift_matrices():
    x, at = np.indices((W, W))
    col = at % HALF
    near = x // 2
    far = np.clip(near + 2 * (x % 2) - 1, 0, HALF - 1)
    base = 0.75 * (col == near) + 0.25 * (col == far)
    second = at // HALF == 1
    return np.stack([base * np.where(second, 0.75, 0.25), base * np.where(second, 0.25, 0.75)]).astype(np.float32)


def stage_one(m0_ref, m1_ref, m2_ref, m3_ref, w1_ref, mid_ref, pad_s, in_s):
    clear_pads(pad_s)

    def frame(f, _):
        for r, ref in enumerate((m0_ref, m1_ref, m2_ref, m3_ref)):
            shifted(relu(ref[f, :W]), pad_s.at[r], in_s, r)
        for j in range(2):
            mid_ref[f, j] = relu(taps(in_s, j, w1_ref)).astype(BF16)
        return 0

    lax.fori_loop(0, m0_ref.shape[0], frame, 0)


def stage_two(side, halo_ref, near_ref, far_ref, mid_ref, coarse_ref, lift_ref, w1_ref, w2_ref,
              inner_ref, first_ref, second_ref, pad_s, in_s, mid_s, coarse_s):
    edge = lax.axis_index("space") == side * (lax.axis_size("space") - 1)
    steps = (0, 1) if side else (1, 2)
    order = 1 - 2 * side
    clear_pads(pad_s)

    def frame(f, _):
        own = coarse_ref[f, side]
        coarse_s[side * HALF:(side + 1) * HALF] = jnp.where(edge, own, halo_ref[f, W:])
        coarse_s[(1 - side) * HALF:(2 - side) * HALF] = own
        for r, ref in enumerate((halo_ref, near_ref, far_ref)[::order]):
            shifted(relu(ref[f, :W]), pad_s.at[r], in_s, r)
        for j in range(2):
            shifted(mid_ref[f, j], pad_s.at[3 + j], mid_s, j + 1 - side)
        shifted(relu(taps(in_s, 0, w1_ref)).astype(BF16), pad_s.at[5], mid_s, 2 * side)
        first_ref[f] = taps(in_s, side, w1_ref, None, steps)
        total = taps(mid_s, 0, w2_ref, dot(lift_ref[1 - side], coarse_ref[f].reshape(2 * HALF, C)))
        inner_ref[f] = (total + far_ref[f, :W].astype(F32)).astype(BF16)
        total = taps(mid_s, side, w2_ref, dot(lift_ref[side], coarse_s[...]), steps)
        second_ref[f] = total + near_ref[f, :W].astype(F32)
        return 0

    lax.fori_loop(0, near_ref.shape[0], frame, 0)


def stage_three(side, halo_ref, inner_ref, first_ref, second_ref, w1_ref, w2_ref, *rest):
    out_hbm, pad_s, in_s, mid_s, row_s, sems = rest[-6:]
    edge = lax.axis_index("space") == side * (lax.axis_size("space") - 1)
    frames = halo_ref.shape[0]
    copies = [pltpu.make_async_copy(inner_ref.at[f], out_hbm.at[f, 1 + side], sems.at[f]) for f in range(frames)]
    copies += [pltpu.make_async_copy(row_s.at[f], out_hbm.at[f, 3 * side], sems.at[frames + f]) for f in range(frames)]
    for copy in copies[:frames]:
        copy.start()
    clear_pads(pad_s)
    step = (2 * side,)
    for f in range(frames):
        shifted(relu(halo_ref[f]), pad_s.at[f], in_s, f)
        value = relu(taps(in_s, f, w1_ref, first_ref[f], step)).astype(BF16)
        value = jnp.where(edge, jnp.zeros_like(value), value)
        shifted(value, pad_s.at[frames + f], mid_s, f)
        row_s[f] = taps(mid_s, f, w2_ref, second_ref[f], step).astype(BF16)
        copies[frames + f].start()
    for copy in copies:
        copy.wait()


def last_stage(side, name, args, out, rows):
    frames = args[0].shape[0]
    before = [] if out is None else [out]
    return pl.pallas_call(
        functools.partial(stage_three, side),
        in_specs=[pl.BlockSpec(memory_space=pltpu.VMEM)] * len(args)
        + [pl.BlockSpec(memory_space=pltpu.HBM)] * len(before),
        out_specs=pl.BlockSpec(memory_space=pltpu.HBM),
        out_shape=jax.ShapeDtypeStruct((frames, rows, W, C), BF16),
        scratch_shapes=[pads(2 * frames), planes(frames), planes(frames), pltpu.VMEM((frames, W, C), BF16),
                        pltpu.SemaphoreType.DMA((2 * frames,))],
        input_output_aliases={len(args): 0} if before else {},
        compiler_params=pltpu.CompilerParams(vmem_limit_bytes=VMEM_LIMIT),
        cost_estimate=pl.CostEstimate(flops=2 * 10**9, transcendentals=0, bytes_accessed=1 << 20),
        name=name,
    )(*args, *before)


def planes(rows):
    return pltpu.VMEM((3, rows * W, C), BF16)


def pads(rows):
    return pltpu.VMEM((rows, W + 16, C), F32)


def local(fine, coarse, w_query, w_key, w_value, w_out, conv_first, conv_second):
    frames = fine.shape[0]
    size = lax.axis_size("space")
    up = [(i, i + 1) for i in range(size - 1)]
    down = [(i + 1, i) for i in range(size - 1)]
    other = lax.ppermute(fine, "tm", [(0, 1), (1, 0)])
    pos = jnp.asarray(encode_table(2 * frames, C))
    ready = own_projections(pos, fine, w_query, w_key, w_value, w_out)
    held_pos, held, wqkv, wo, q, k, v = ready
    m0, m3 = attention(outer_body, "attention_outer", (held_pos, held, other, wqkv, wo, q, k, v, coarse), W + HALF,
                       [], 5)
    above = lax.ppermute(m3, "space", up)
    below = lax.ppermute(m0, "space", down)
    wide = pltpu.VMEM((1, frames, C, W), F32)
    m1, m2 = attention(inner_body, "attention_inner", (held_pos, held, other, wqkv, wo, m0), W, [wide] * 3, 7)
    above2 = lax.ppermute(m2, "space", up)
    below2 = lax.ppermute(m1, "space", down)
    (mid,) = call(stage_one, "stage_one", (m0, m1, m2, m3, conv_first), [((frames, 2, W, C), BF16)],
                  [pads(4), planes(4)], 3)
    row = (frames, W, C)
    lift = jnp.asarray(lift_matrices(), BF16)
    parts = []
    for side, (halo, near, far) in enumerate(((above, m0, m1), (below, m3, m2))):
        parts.append(call(functools.partial(stage_two, side), "stage_two_%d" % side,
                          (halo, near, far, mid, coarse, lift, conv_first, conv_second),
                          [(row, BF16), (row, F32), (row, F32)],
                          [pads(6), planes(3), planes(3), pltpu.VMEM((2 * HALF, C), BF16)], 5))
    out = None
    for side, halo in enumerate((above2, below2)):
        out = last_stage(side, "stage_three_%d" % side, (halo, *parts[side], conv_first, conv_second, parts[1 - side][0]),
                         out, fine.shape[1])
    return out


def solution(mesh):
    split = P("tm", "space", None, None)
    return jax.shard_map(
        local,
        mesh=mesh,
        in_specs=(split, split, P(), P(), P(), P(), P(), P()),
        out_specs=split,
        check_vma=False,
    )
```

```python
import functools

import jax
import jax.numpy as jnp
import numpy as np
from jax import lax
from jax.experimental import pallas as pl
from jax.experimental.pallas import tpu as pltpu
from jax.sharding import PartitionSpec as P

HEADS = 8
C = 256
D = C // HEADS
W = 256
HALF = W // 2
F32 = jnp.float32
BF16 = jnp.bfloat16
VMEM_LIMIT = 20 * 1024 * 1024


def encode_table(frames, width):
    half = width // 2
    inverse = np.exp(-np.log(10000.0) * 2.0 * np.arange(half) / width)
    angles = np.arange(frames)[:, None] * inverse[None, :]
    table = np.concatenate([np.sin(angles), np.cos(angles)], axis=1).astype(np.float32)
    return np.ascontiguousarray(np.broadcast_to(table[:, :, None], (frames, width, 128)))


def dot(a, b):
    return jnp.dot(a, b, preferred_element_type=F32)


def normed_row(x_ref, i, row, pos, norm):
    for half in range(W // 128):
        lanes = slice(half * 128, half * 128 + 128)
        h = x_ref[i, row, lanes, :].T.astype(F32) + pos
        center = h - jnp.sum(h, axis=0, keepdims=True) * (1.0 / C)
        spread = jnp.sum(center * center, axis=0, keepdims=True) * (1.0 / C)
        norm[:, lanes] = (center * lax.rsqrt(spread + 1e-05)).astype(BF16)


def own_row(at_row, row, pos_ref, own_ref, wqkv_ref, q_ref, k_ref, v_ref, norm_s):
    frames = own_ref.shape[0]
    base = lax.axis_index("tm") * frames
    for f in range(frames):
        norm = norm_s.at[at_row * frames + f]
        normed_row(own_ref, f, row, pos_ref[base + f], norm)
        y = dot(wqkv_ref[...], norm[...])
        q_ref[at_row, f] = y[:C]
        k_ref[at_row, f] = y[C:2 * C]
        v_ref[at_row, f] = y[2 * C:]


def other_row(n, row, pos_ref, other_ref, wqkv_ref, norm_s, k_s, v_s):
    frames = other_ref.shape[0]
    base = (1 - lax.axis_index("tm")) * frames
    for f in range(frames):
        norm = norm_s.at[n * frames + f]
        normed_row(other_ref, f, row, pos_ref[base + f], norm)
        y = dot(wqkv_ref[C:], norm[...])
        k_s[n, f] = y[:C]
        v_s[n, f] = y[C:]


def scores(n, lanes, q_ref, key_refs):
    frames = q_ref.shape[1]

    def step(d, acc):
        at = pl.ds(pl.multiple_of(d * HEADS, HEADS), HEADS)
        qs = [q_ref[n, a, at, lanes] for a in range(frames)]
        ks = [ref[n, b, at, lanes] for ref in key_refs for b in range(frames)]
        return tuple(total + q * k for total, (q, k) in zip(acc, [(q, k) for q in qs for k in ks]))

    zero = jnp.zeros((HEADS, 128), F32)
    return lax.fori_loop(0, D, step, (zero,) * (frames * frames * len(key_refs)), unroll=16 // len(key_refs))


def attend_row(n, q_ref, ko_ref, vo_ref, k_s, v_s, att_s, prior_ref=None):
    frames = q_ref.shape[1]
    keys = 2 * frames
    factor = float(np.log2(np.e) / np.sqrt(D))
    for half in range(W // 128):
        lanes = slice(half * 128, half * 128 + 128)
        if prior_ref is None:
            acc = scores(n, lanes, q_ref, (ko_ref, k_s))
        else:
            late = scores(n, lanes, q_ref, (k_s,))
            acc = []
            for a in range(frames):
                acc += [prior_ref[n, half, a * frames + b] for b in range(frames)]
                acc += late[a * frames:(a + 1) * frames]
        weights = []
        for a in range(frames):
            line = acc[a * keys:(a + 1) * keys]
            top = line[0]
            for s in line[1:]:
                top = jnp.maximum(top, s)
            powers = [jnp.exp2((s - top) * factor) for s in line]
            total = powers[0]
            for p in powers[1:]:
                total = total + p
            inv = 1.0 / total
            weights += [p * inv for p in powers]

        def gather(d2, _):
            outs = [[] for _ in range(frames)]
            for sub in range(2):
                at = pl.ds(pl.multiple_of(d2 * 2 * HEADS + sub * HEADS, HEADS), HEADS)
                vs = [vo_ref[n, b, at, lanes] for b in range(frames)] + [v_s[n, b, at, lanes] for b in range(frames)]
                for a in range(frames):
                    total = weights[a * keys] * vs[0]
                    for b in range(1, keys):
                        total = total + weights[a * keys + b] * vs[b]
                    outs[a].append(total)
            at = pl.ds(pl.multiple_of(d2 * 2 * HEADS, 2 * HEADS), 2 * HEADS)
            for a in range(frames):
                att_s[n, a, at, lanes] = jnp.concatenate(outs[a], axis=0).astype(BF16)
            return 0

        lax.fori_loop(0, D // 2, gather, 0, unroll=4)


def out_row(n, row, own_ref, wo_ref, att_s, out_ref):
    for a in range(own_ref.shape[0]):
        branch = lax.dot_general(att_s[n, a], wo_ref[...], (((0,), (0,)), ((), ())), preferred_element_type=F32)
        out_ref[a, :W] = (own_ref[a, row].astype(F32) + branch).astype(BF16)


def own_body(pos_hbm, own_hbm, wq_hbm, wk_hbm, wv_hbm, wo_hbm,
             pos_ref, own_ref, wqkv_ref, wor_ref, q_ref, k_ref, v_ref, prior_ref, w_s, norm_s, sems):
    frames, rows = own_hbm.shape[:2]
    loads = [pltpu.make_async_copy(ref, w_s.at[n], sems.at[n]) for n, ref in enumerate((wq_hbm, wk_hbm, wv_hbm, wo_hbm))]
    loads.append(pltpu.make_async_copy(pos_hbm, pos_ref, sems.at[4]))
    loads.append(pltpu.make_async_copy(own_hbm, own_ref, sems.at[5]))
    for load in loads:
        load.start()
    to = lax.broadcasted_iota(jnp.int32, (C, C), 0)
    at = lax.broadcasted_iota(jnp.int32, (C, C), 1)
    pick = (at == (to % HEADS) * D + to // HEADS).astype(BF16)
    nt = (((1,), (1,)), ((), ()))
    for load in loads[:4]:
        load.wait()
    for n in range(3):
        wqkv_ref[n * C:(n + 1) * C] = lax.dot_general(pick, w_s[n], nt, preferred_element_type=F32).astype(BF16)
    wor_ref[...] = dot(pick, w_s[3]).astype(BF16)
    for load in loads[4:]:
        load.wait()
    for n, row in enumerate((0, own_ref.shape[1] - 1)):
        own_row(n, row, pos_ref, own_ref, wqkv_ref, q_ref, k_ref, v_ref, norm_s)
    for n in range(2):
        for half in range(W // 128):
            lanes = slice(half * 128, half * 128 + 128)
            for i, total in enumerate(scores(n, lanes, q_ref, (k_ref,))):
                prior_ref[n, half, i] = total


def outer_body(pos_ref, own_ref, other_ref, wqkv_ref, wo_ref, q_ref, k_ref, v_ref, prior_ref, coarse_ref,
               down_ref, up_ref, norm_s, k_s, v_s, att_s):
    rows = (0, own_ref.shape[1] - 1)
    for n, row in enumerate(rows):
        other_row(n, row, pos_ref, other_ref, wqkv_ref, norm_s, k_s, v_s)
    for n in range(2):
        attend_row(n, q_ref, k_ref, v_ref, k_s, v_s, att_s, prior_ref)
    for n, (row, ref) in enumerate(zip(rows, (down_ref, up_ref))):
        out_row(n, row, own_ref, wo_ref, att_s, ref)
        ref[:, W:] = coarse_ref[:, n * (coarse_ref.shape[1] - 1)]


def inner_body(pos_ref, own_ref, other_ref, wqkv_ref, wo_ref, before_ref, down_ref, up_ref,
               norm_s, k_s, v_s, att_s, q_s, ko_s, vo_s, normo_s):
    del before_ref
    rows = (1, own_ref.shape[1] - 2)
    for n, row in enumerate(rows):
        own_row(n, row, pos_ref, own_ref, wqkv_ref, q_s, ko_s, vo_s, normo_s)
        other_row(n, row, pos_ref, other_ref, wqkv_ref, norm_s, k_s, v_s)
    for n in range(2):
        attend_row(n, q_s, ko_s, vo_s, k_s, v_s, att_s)
    for n, (row, ref) in enumerate(zip(rows, (down_ref, up_ref))):
        out_row(n, row, own_ref, wo_ref, att_s, ref)


def call(body, name, args, outs, scratch, micros, space=pltpu.VMEM):
    return pl.pallas_call(
        body,
        in_specs=[pl.BlockSpec(memory_space=space)] * len(args),
        out_specs=[pl.BlockSpec(memory_space=pltpu.VMEM)] * len(outs),
        out_shape=[jax.ShapeDtypeStruct(s, t) for s, t in outs],
        scratch_shapes=scratch,
        compiler_params=pltpu.CompilerParams(vmem_limit_bytes=VMEM_LIMIT),
        cost_estimate=pl.CostEstimate(flops=micros * 10**9, transcendentals=0, bytes_accessed=1 << 20),
        name=name,
    )(*args)


def own_projections(pos, own, *weights):
    frames, rows = own.shape[:2]
    wide = ((2, frames, C, W), F32)
    args = [pltpu.with_memory_space_constraint(a, pltpu.HBM) for a in (pos, own, *weights)]
    return call(own_body, "own_projections", args,
                [(pos.shape, F32), (own.shape, BF16), ((3 * C, C), BF16), ((C, C), BF16), wide, wide, wide,
                 ((2, W // 128, frames * frames, HEADS, 128), F32)],
                [pltpu.VMEM((4, C, C), BF16), pltpu.VMEM((2 * frames, C, W), BF16), pltpu.SemaphoreType.DMA((6,))], 6, pltpu.HBM)


def attention(body, name, args, width, extra, micros):
    frames = args[1].shape[0]
    return call(body, name, args, [((frames, width, C), BF16)] * 2,
                [pltpu.VMEM((2 * frames, C, W), BF16), pltpu.VMEM((2, frames, C, W), F32),
                 pltpu.VMEM((2, frames, C, W), F32), pltpu.VMEM((2, frames, C, W), BF16)] + extra, micros)


def clear_pads(pad_s):
    for r in range(pad_s.shape[0]):
        pad_s[r, 0:8] = jnp.zeros((8, C), F32)
        pad_s[r, 8 + W:16 + W] = jnp.zeros((8, C), F32)


def shifted(value, pad, out_s, row):
    pad[8:8 + W] = value.astype(F32)
    at = slice(row * W, (row + 1) * W)
    out_s[1, at] = value
    out_s[0, at] = pad[7:7 + W].astype(BF16)
    out_s[2, at] = pad[9:9 + W].astype(BF16)


def taps(source_s, row, w_ref, total=None, steps=(0, 1, 2)):
    for n, dy in enumerate(steps):
        for dx in range(3):
            part = dot(source_s[dx, (row + n) * W:(row + n + 1) * W], w_ref[dy, dx])
            total = part if total is None else total + part
    return total


def relu(value):
    return jnp.maximum(value, jnp.zeros((), value.dtype))


def lift_matrices():
    x, at = np.indices((W, W))
    col = at % HALF
    near = x // 2
    far = np.clip(near + 2 * (x % 2) - 1, 0, HALF - 1)
    base = 0.75 * (col == near) + 0.25 * (col == far)
    second = at // HALF == 1
    return np.stack([base * np.where(second, 0.75, 0.25), base * np.where(second, 0.25, 0.75)]).astype(np.float32)


def stage_one(m0_ref, m1_ref, m2_ref, m3_ref, w1_ref, mid_ref, pad_s, in_s):
    clear_pads(pad_s)

    def frame(f, _):
        for r, ref in enumerate((m0_ref, m1_ref, m2_ref, m3_ref)):
            shifted(relu(ref[f, :W]), pad_s.at[r], in_s, r)
        for j in range(2):
            mid_ref[f, j] = relu(taps(in_s, j, w1_ref)).astype(BF16)
        return 0

    lax.fori_loop(0, m0_ref.shape[0], frame, 0)


def stage_two(side, halo_ref, near_ref, far_ref, mid_ref, coarse_ref, lift_ref, w1_ref, w2_ref,
              inner_ref, first_ref, second_ref, pad_s, in_s, mid_s, coarse_s):
    edge = lax.axis_index("space") == side * (lax.axis_size("space") - 1)
    steps = (0, 1) if side else (1, 2)
    order = 1 - 2 * side
    clear_pads(pad_s)

    def frame(f, _):
        own = coarse_ref[f, side]
        coarse_s[side * HALF:(side + 1) * HALF] = jnp.where(edge, own, halo_ref[f, W:])
        coarse_s[(1 - side) * HALF:(2 - side) * HALF] = own
        for r, ref in enumerate((halo_ref, near_ref, far_ref)[::order]):
            shifted(relu(ref[f, :W]), pad_s.at[r], in_s, r)
        for j in range(2):
            shifted(mid_ref[f, j], pad_s.at[3 + j], mid_s, j + 1 - side)
        shifted(relu(taps(in_s, 0, w1_ref)).astype(BF16), pad_s.at[5], mid_s, 2 * side)
        first_ref[f] = taps(in_s, side, w1_ref, None, steps)
        total = taps(mid_s, 0, w2_ref, dot(lift_ref[1 - side], coarse_ref[f].reshape(2 * HALF, C)))
        inner_ref[f] = (total + far_ref[f, :W].astype(F32)).astype(BF16)
        total = taps(mid_s, side, w2_ref, dot(lift_ref[side], coarse_s[...]), steps)
        second_ref[f] = total + near_ref[f, :W].astype(F32)
        return 0

    lax.fori_loop(0, near_ref.shape[0], frame, 0)


def stage_three(side, halo_ref, inner_ref, first_ref, second_ref, w1_ref, w2_ref, *rest):
    out_hbm, pad_s, in_s, mid_s, row_s, sems = rest[-6:]
    edge = lax.axis_index("space") == side * (lax.axis_size("space") - 1)
    frames = halo_ref.shape[0]
    copies = [pltpu.make_async_copy(inner_ref.at[f], out_hbm.at[f, 1 + side], sems.at[f]) for f in range(frames)]
    copies += [pltpu.make_async_copy(row_s.at[f], out_hbm.at[f, 3 * side], sems.at[frames + f]) for f in range(frames)]
    for copy in copies[:frames]:
        copy.start()
    clear_pads(pad_s)
    step = (2 * side,)
    for f in range(frames):
        shifted(relu(halo_ref[f]), pad_s.at[f], in_s, f)
        value = relu(taps(in_s, f, w1_ref, first_ref[f], step)).astype(BF16)
        value = jnp.where(edge, jnp.zeros_like(value), value)
        shifted(value, pad_s.at[frames + f], mid_s, f)
        row_s[f] = taps(mid_s, f, w2_ref, second_ref[f], step).astype(BF16)
        copies[frames + f].start()
    for copy in copies:
        copy.wait()


def last_stage(side, name, args, out, rows):
    frames = args[0].shape[0]
    before = [] if out is None else [out]
    return pl.pallas_call(
        functools.partial(stage_three, side),
        in_specs=[pl.BlockSpec(memory_space=pltpu.VMEM)] * len(args)
        + [pl.BlockSpec(memory_space=pltpu.HBM)] * len(before),
        out_specs=pl.BlockSpec(memory_space=pltpu.HBM),
        out_shape=jax.ShapeDtypeStruct((frames, rows, W, C), BF16),
        scratch_shapes=[pads(2 * frames), planes(frames), planes(frames), pltpu.VMEM((frames, W, C), BF16),
                        pltpu.SemaphoreType.DMA((2 * frames,))],
        input_output_aliases={len(args): 0} if before else {},
        compiler_params=pltpu.CompilerParams(vmem_limit_bytes=VMEM_LIMIT),
        cost_estimate=pl.CostEstimate(flops=2 * 10**9, transcendentals=0, bytes_accessed=1 << 20),
        name=name,
    )(*args, *before)


def planes(rows):
    return pltpu.VMEM((3, rows * W, C), BF16)


def pads(rows):
    return pltpu.VMEM((rows, W + 16, C), F32)


def local(fine, coarse, w_query, w_key, w_value, w_out, conv_first, conv_second):
    frames = fine.shape[0]
    size = lax.axis_size("space")
    up = [(i, i + 1) for i in range(size - 1)]
    down = [(i + 1, i) for i in range(size - 1)]
    other = lax.ppermute(fine, "tm", [(0, 1), (1, 0)])
    pos = jnp.asarray(encode_table(2 * frames, C))
    ready = own_projections(pos, fine, w_query, w_key, w_value, w_out)
    held_pos, held, wqkv, wo, *early = ready
    m0, m3 = attention(outer_body, "attention_outer", (held_pos, held, other, wqkv, wo, *early, coarse), W + HALF,
                       [], 5)
    above = lax.ppermute(m3, "space", up)
    below = lax.ppermute(m0, "space", down)
    wide = pltpu.VMEM((2, frames, C, W), F32)
    m1, m2 = attention(inner_body, "attention_inner", (held_pos, held, other, wqkv, wo, m0), W,
                       [wide] * 3 + [pltpu.VMEM((2 * frames, C, W), BF16)], 7)
    above2 = lax.ppermute(m2, "space", up)
    below2 = lax.ppermute(m1, "space", down)
    (mid,) = call(stage_one, "stage_one", (m0, m1, m2, m3, conv_first), [((frames, 2, W, C), BF16)],
                  [pads(4), planes(4)], 3)
    row = (frames, W, C)
    lift = jnp.asarray(lift_matrices(), BF16)
    parts = []
    for side, (halo, near, far) in enumerate(((above, m0, m1), (below, m3, m2))):
        parts.append(call(functools.partial(stage_two, side), "stage_two_%d" % side,
                          (halo, near, far, mid, coarse, lift, conv_first, conv_second),
                          [(row, BF16), (row, F32), (row, F32)],
                          [pads(6), planes(3), planes(3), pltpu.VMEM((2 * HALF, C), BF16)], 5))
    out = None
    for side, halo in enumerate((above2, below2)):
        out = last_stage(side, "stage_three_%d" % side, (halo, *parts[side], conv_first, conv_second, parts[1 - side][0]),
                         out, fine.shape[1])
    return out


def solution(mesh):
    split = P("tm", "space", None, None)
    return jax.shard_map(
        local,
        mesh=mesh,
        in_specs=(split, split, P(), P(), P(), P(), P(), P()),
        out_specs=split,
        check_vma=False,
    )
```

```python
import functools

import jax
import jax.numpy as jnp
import numpy as np
from jax import lax
from jax.experimental import pallas as pl
from jax.experimental.pallas import tpu as pltpu
from jax.sharding import PartitionSpec as P

HEADS = 8
C = 256
D = C // HEADS
W = 256
HALF = W // 2
F32 = jnp.float32
BF16 = jnp.bfloat16
VMEM_LIMIT = 20 * 1024 * 1024


def encode_table(frames, width):
    half = width // 2
    inverse = np.exp(-np.log(10000.0) * 2.0 * np.arange(half) / width)
    angles = np.arange(frames)[:, None] * inverse[None, :]
    table = np.concatenate([np.sin(angles), np.cos(angles)], axis=1).astype(np.float32)
    return np.ascontiguousarray(np.broadcast_to(table[:, :, None], (frames, width, 128)))


def flip():
    return (lax.axis_index("space") + 1) % 2


def dot(a, b):
    return jnp.dot(a, b, preferred_element_type=F32)


def normed_row(x_ref, i, row, pos, norm):
    for half in range(W // 128):
        lanes = slice(half * 128, half * 128 + 128)
        h = x_ref[i, row, lanes, :].T.astype(F32) + pos
        center = h - jnp.sum(h, axis=0, keepdims=True) * (1.0 / C)
        spread = jnp.sum(center * center, axis=0, keepdims=True) * (1.0 / C)
        norm[:, lanes] = (center * lax.rsqrt(spread + 1e-05)).astype(BF16)


def own_row(at_row, row, pos_ref, own_ref, wqkv_ref, q_ref, k_ref, v_ref, norm_s):
    frames = own_ref.shape[0]
    base = lax.axis_index("tm") * frames
    for f in range(frames):
        norm = norm_s.at[at_row * frames + f]
        normed_row(own_ref, f, row, pos_ref[base + f], norm)
        y = dot(wqkv_ref[...], norm[...])
        q_ref[at_row, f] = y[:C]
        k_ref[at_row, f] = y[C:2 * C]
        v_ref[at_row, f] = y[2 * C:]


def other_row(n, row, pos_ref, other_ref, wqkv_ref, norm_s, k_s, v_s):
    frames = other_ref.shape[0]
    base = (1 - lax.axis_index("tm")) * frames
    for f in range(frames):
        norm = norm_s.at[n * frames + f]
        normed_row(other_ref, f, row, pos_ref[base + f], norm)
        y = dot(wqkv_ref[C:], norm[...])
        k_s[n, f] = y[:C]
        v_s[n, f] = y[C:]


def scores(n, lanes, q_ref, key_refs):
    frames = q_ref.shape[1]

    def step(d, acc):
        at = pl.ds(pl.multiple_of(d * HEADS, HEADS), HEADS)
        qs = [q_ref[n, a, at, lanes] for a in range(frames)]
        ks = [ref[n, b, at, lanes] for ref in key_refs for b in range(frames)]
        return tuple(total + q * k for total, (q, k) in zip(acc, [(q, k) for q in qs for k in ks]))

    zero = jnp.zeros((HEADS, 128), F32)
    return lax.fori_loop(0, D, step, (zero,) * (frames * frames * len(key_refs)), unroll=16 // len(key_refs))


def attend_row(n, q_ref, ko_ref, vo_ref, k_s, v_s, att_s, prior_ref=None):
    frames = q_ref.shape[1]
    keys = 2 * frames
    factor = float(np.log2(np.e) / np.sqrt(D))
    for half in range(W // 128):
        lanes = slice(half * 128, half * 128 + 128)
        if prior_ref is None:
            acc = scores(n, lanes, q_ref, (ko_ref, k_s))
        else:
            late = scores(n, lanes, q_ref, (k_s,))
            acc = []
            for a in range(frames):
                acc += [prior_ref[n, half, a * frames + b] for b in range(frames)]
                acc += late[a * frames:(a + 1) * frames]
        weights = []
        for a in range(frames):
            line = acc[a * keys:(a + 1) * keys]
            top = line[0]
            for s in line[1:]:
                top = jnp.maximum(top, s)
            powers = [jnp.exp2((s - top) * factor) for s in line]
            total = powers[0]
            for p in powers[1:]:
                total = total + p
            inv = 1.0 / total
            weights += [p * inv for p in powers]

        def gather(d2, _):
            outs = [[] for _ in range(frames)]
            for sub in range(2):
                at = pl.ds(pl.multiple_of(d2 * 2 * HEADS + sub * HEADS, HEADS), HEADS)
                vs = [vo_ref[n, b, at, lanes] for b in range(frames)] + [v_s[n, b, at, lanes] for b in range(frames)]
                for a in range(frames):
                    total = weights[a * keys] * vs[0]
                    for b in range(1, keys):
                        total = total + weights[a * keys + b] * vs[b]
                    outs[a].append(total)
            at = pl.ds(pl.multiple_of(d2 * 2 * HEADS, 2 * HEADS), 2 * HEADS)
            for a in range(frames):
                att_s[n, a, at, lanes] = jnp.concatenate(outs[a], axis=0).astype(BF16)
            return 0

        lax.fori_loop(0, D // 2, gather, 0, unroll=4)


def out_row(n, row, own_ref, wo_ref, att_s, out_ref):
    for a in range(own_ref.shape[0]):
        branch = lax.dot_general(att_s[n, a], wo_ref[...], (((0,), (0,)), ((), ())), preferred_element_type=F32)
        out_ref[a, :W] = (own_ref[a, row].astype(F32) + branch).astype(BF16)


def own_body(pos_hbm, own_hbm, wq_hbm, wk_hbm, wv_hbm, wo_hbm,
             pos_ref, own_ref, wqkv_ref, wor_ref, q_ref, k_ref, v_ref, prior_ref, w_s, norm_s, sems):
    frames, rows = own_hbm.shape[:2]
    loads = [pltpu.make_async_copy(ref, w_s.at[n], sems.at[n]) for n, ref in enumerate((wq_hbm, wk_hbm, wv_hbm, wo_hbm))]
    loads.append(pltpu.make_async_copy(pos_hbm, pos_ref, sems.at[4]))
    loads.append(pltpu.make_async_copy(own_hbm, own_ref, sems.at[5]))
    for load in loads:
        load.start()
    to = lax.broadcasted_iota(jnp.int32, (C, C), 0)
    at = lax.broadcasted_iota(jnp.int32, (C, C), 1)
    pick = (at == (to % HEADS) * D + to // HEADS).astype(BF16)
    nt = (((1,), (1,)), ((), ()))
    for load in loads[:4]:
        load.wait()
    for n in range(3):
        wqkv_ref[n * C:(n + 1) * C] = lax.dot_general(pick, w_s[n], nt, preferred_element_type=F32).astype(BF16)
    wor_ref[...] = dot(pick, w_s[3]).astype(BF16)
    for load in loads[4:]:
        load.wait()
    start, last = flip() * (own_ref.shape[1] - 1), own_ref.shape[1] - 1
    for n, row in enumerate((start, last - start)):
        own_row(n, row, pos_ref, own_ref, wqkv_ref, q_ref, k_ref, v_ref, norm_s)
    for n in range(2):
        for half in range(W // 128):
            lanes = slice(half * 128, half * 128 + 128)
            for i, total in enumerate(scores(n, lanes, q_ref, (k_ref,))):
                prior_ref[n, half, i] = total


def outer_body(pos_ref, own_ref, other_ref, wqkv_ref, wo_ref, q_ref, k_ref, v_ref, prior_ref,
               down_ref, up_ref, norm_s, k_s, v_s, att_s):
    start, last = flip() * (own_ref.shape[1] - 1), own_ref.shape[1] - 1
    rows = (start, last - start)
    for n, row in enumerate(rows):
        other_row(n, row, pos_ref, other_ref, wqkv_ref, norm_s, k_s, v_s)
    for n in range(2):
        attend_row(n, q_ref, k_ref, v_ref, k_s, v_s, att_s, prior_ref)
    for n, (row, ref) in enumerate(zip(rows, (down_ref, up_ref))):
        out_row(n, row, own_ref, wo_ref, att_s, ref)


def inner_body(pos_ref, own_ref, other_ref, wqkv_ref, wo_ref, coarse_ref, before_ref, down_ref, up_ref,
               norm_s, k_s, v_s, att_s, q_s, ko_s, vo_s, normo_s):
    del before_ref
    start = 1 + flip() * (own_ref.shape[1] - 3)
    rows = (start, own_ref.shape[1] - 1 - start)
    for n, row in enumerate(rows):
        own_row(n, row, pos_ref, own_ref, wqkv_ref, q_s, ko_s, vo_s, normo_s)
        other_row(n, row, pos_ref, other_ref, wqkv_ref, norm_s, k_s, v_s)
    for n in range(2):
        attend_row(n, q_s, ko_s, vo_s, k_s, v_s, att_s)
    for n, (row, ref) in enumerate(zip(rows, (down_ref, up_ref))):
        out_row(n, row, own_ref, wo_ref, att_s, ref)
        ref[:, W:] = coarse_ref[:, flip() ^ n]


def call(body, name, args, outs, scratch, micros, space=pltpu.VMEM):
    return pl.pallas_call(
        body,
        in_specs=[pl.BlockSpec(memory_space=space)] * len(args),
        out_specs=[pl.BlockSpec(memory_space=pltpu.VMEM)] * len(outs),
        out_shape=[jax.ShapeDtypeStruct(s, t) for s, t in outs],
        scratch_shapes=scratch,
        compiler_params=pltpu.CompilerParams(vmem_limit_bytes=VMEM_LIMIT),
        cost_estimate=pl.CostEstimate(flops=micros * 10**9, transcendentals=0, bytes_accessed=1 << 20),
        name=name,
    )(*args)


def own_projections(pos, own, *weights):
    frames, rows = own.shape[:2]
    wide = ((2, frames, C, W), F32)
    args = [pltpu.with_memory_space_constraint(a, pltpu.HBM) for a in (pos, own, *weights)]
    return call(own_body, "own_projections", args,
                [(pos.shape, F32), (own.shape, BF16), ((3 * C, C), BF16), ((C, C), BF16), wide, wide, wide,
                 ((2, W // 128, frames * frames, HEADS, 128), F32)],
                [pltpu.VMEM((4, C, C), BF16), pltpu.VMEM((2 * frames, C, W), BF16), pltpu.SemaphoreType.DMA((6,))], 6, pltpu.HBM)


def attention(body, name, args, width, extra, micros):
    frames = args[1].shape[0]
    return call(body, name, args, [((frames, width, C), BF16)] * 2,
                [pltpu.VMEM((2 * frames, C, W), BF16), pltpu.VMEM((2, frames, C, W), F32),
                 pltpu.VMEM((2, frames, C, W), F32), pltpu.VMEM((2, frames, C, W), BF16)] + extra, micros)


def clear_pads(pad_s):
    for r in range(pad_s.shape[0]):
        pad_s[r, 0:8] = jnp.zeros((8, C), F32)
        pad_s[r, 8 + W:16 + W] = jnp.zeros((8, C), F32)


def shifted(value, pad, out_s, row):
    pad[8:8 + W] = value.astype(F32)
    at = slice(row * W, (row + 1) * W)
    out_s[1, at] = value
    out_s[0, at] = pad[7:7 + W].astype(BF16)
    out_s[2, at] = pad[9:9 + W].astype(BF16)


def taps(source_s, row, w_ref, total=None, steps=(0, 1, 2)):
    turned = flip()
    for n, dy in enumerate(steps):
        tap = dy + turned * (2 - 2 * dy)
        for dx in range(3):
            part = dot(source_s[dx, (row + n) * W:(row + n + 1) * W], w_ref[tap, dx])
            total = part if total is None else total + part
    return total


def relu(value):
    return jnp.maximum(value, jnp.zeros((), value.dtype))


def lift_matrices():
    x, at = np.indices((W, W))
    col = at % HALF
    near = x // 2
    far = np.clip(near + 2 * (x % 2) - 1, 0, HALF - 1)
    base = 0.75 * (col == near) + 0.25 * (col == far)
    second = at // HALF == 1
    return np.stack([base * np.where(second, 0.75, 0.25), base * np.where(second, 0.25, 0.75)]).astype(np.float32)


def stage_one(m0_ref, m1_ref, m2_ref, m3_ref, w1_ref, mid_ref, pad_s, in_s):
    clear_pads(pad_s)

    def frame(f, _):
        for r, ref in enumerate((m0_ref, m1_ref, m2_ref, m3_ref)):
            shifted(relu(ref[f, :W]), pad_s.at[r], in_s, r)
        for j in range(2):
            mid_ref[f, j] = relu(taps(in_s, j, w1_ref)).astype(BF16)
        return 0

    lax.fori_loop(0, m0_ref.shape[0], frame, 0)


def at_edge(side):
    here = lax.axis_index("space")
    end = (flip() ^ side) * (lax.axis_size("space") - 1)
    return here == end


def stage_two(side, halo_ref, near_ref, far_ref, mid_ref, coarse_ref, lift_ref, w1_ref, w2_ref,
              inner_ref, first_ref, second_ref, pad_s, in_s, mid_s):
    steps = (0, 1) if side else (1, 2)
    order = 1 - 2 * side
    near = flip() ^ side
    clear_pads(pad_s)

    def frame(f, _):
        for r, ref in enumerate((halo_ref, near_ref, far_ref)[::order]):
            shifted(relu(ref[f, :W]), pad_s.at[r], in_s, r)
        for j in range(2):
            shifted(mid_ref[f, j], pad_s.at[3 + j], mid_s, j + 1 - side)
        shifted(relu(taps(in_s, 0, w1_ref)).astype(BF16), pad_s.at[5], mid_s, 2 * side)
        first_ref[f] = taps(in_s, side, w1_ref, None, steps)
        total = taps(mid_s, 0, w2_ref, dot(lift_ref[1 - near], coarse_ref[f].reshape(2 * HALF, C)))
        inner_ref[f] = (total + far_ref[f, :W].astype(F32)).astype(BF16)
        second_ref[f] = taps(mid_s, side, w2_ref, near_ref[f, :W].astype(F32), steps)
        return 0

    lax.fori_loop(0, near_ref.shape[0], frame, 0)


def stage_three(side, halo_ref, coarse_ref, lift_ref, inner_ref, first_ref, second_ref, w1_ref, w2_ref, *rest):
    out_hbm, pad_s, in_s, mid_s, row_s, coarse_s, sems = rest[-7:]
    edge = at_edge(side)
    near = flip() ^ side
    frames = halo_ref.shape[0]
    copies = [pltpu.make_async_copy(inner_ref.at[f], out_hbm.at[f, 1 + near], sems.at[f]) for f in range(frames)]
    copies += [pltpu.make_async_copy(row_s.at[f], out_hbm.at[f, 3 * near], sems.at[frames + f]) for f in range(frames)]
    for copy in copies[:frames]:
        copy.start()
    clear_pads(pad_s)
    step = (2 * side,)
    for f in range(frames):
        shifted(relu(halo_ref[f, :W]), pad_s.at[f], in_s, f)
        own = coarse_ref[f, near]
        coarse_s[f, :HALF] = jnp.where(edge, own, halo_ref[f, W:])
        coarse_s[f, HALF:] = own
        value = relu(taps(in_s, f, w1_ref, first_ref[f], step)).astype(BF16)
        value = jnp.where(edge, jnp.zeros_like(value), value)
        shifted(value, pad_s.at[frames + f], mid_s, f)
        total = second_ref[f] + dot(lift_ref[0], coarse_s[f])
        row_s[f] = taps(mid_s, f, w2_ref, total, step).astype(BF16)
        copies[frames + f].start()
    for copy in copies:
        copy.wait()


def last_stage(side, name, args, out, rows):
    frames = args[0].shape[0]
    before = [] if out is None else [out]
    return pl.pallas_call(
        functools.partial(stage_three, side),
        in_specs=[pl.BlockSpec(memory_space=pltpu.VMEM)] * len(args)
        + [pl.BlockSpec(memory_space=pltpu.HBM)] * len(before),
        out_specs=pl.BlockSpec(memory_space=pltpu.HBM),
        out_shape=jax.ShapeDtypeStruct((frames, rows, W, C), BF16),
        scratch_shapes=[pads(2 * frames), planes(frames), planes(frames), pltpu.VMEM((frames, W, C), BF16),
                        pltpu.VMEM((frames, 2 * HALF, C), BF16), pltpu.SemaphoreType.DMA((2 * frames,))],
        input_output_aliases={len(args): 0} if before else {},
        compiler_params=pltpu.CompilerParams(vmem_limit_bytes=VMEM_LIMIT),
        cost_estimate=pl.CostEstimate(flops=2 * 10**9, transcendentals=0, bytes_accessed=1 << 20),
        name=name,
    )(*args, *before)


def planes(rows):
    return pltpu.VMEM((3, rows * W, C), BF16)


def pads(rows):
    return pltpu.VMEM((rows, W + 16, C), F32)


def local(fine, coarse, w_query, w_key, w_value, w_out, conv_first, conv_second):
    frames = fine.shape[0]
    size = lax.axis_size("space")
    swaps = []
    for first in (0, 1):
        pairs = [(i, i + 1) for i in range(first, size - 1, 2)]
        swaps.append(pairs + [(j, i) for i, j in pairs])
    other = lax.ppermute(fine, "tm", [(0, 1), (1, 0)])
    pos = jnp.asarray(encode_table(2 * frames, C))
    ready = own_projections(pos, fine, w_query, w_key, w_value, w_out)
    held_pos, held, wqkv, wo, *early = ready
    m0, m3 = attention(outer_body, "attention_outer", (held_pos, held, other, wqkv, wo, *early), W,
                       [], 5)
    above, below = [lax.ppermute(m, "space", pairs) for m, pairs in zip((m0, m3), swaps)]
    wide = pltpu.VMEM((2, frames, C, W), F32)
    m1, m2 = attention(inner_body, "attention_inner", (held_pos, held, other, wqkv, wo, coarse, m0), W + HALF,
                       [wide] * 3 + [pltpu.VMEM((2 * frames, C, W), BF16)], 7)
    above2, below2 = [lax.ppermute(m, "space", pairs) for m, pairs in zip((m1, m2), swaps)]
    (mid,) = call(stage_one, "stage_one", (m0, m1, m2, m3, conv_first), [((frames, 2, W, C), BF16)],
                  [pads(4), planes(4)], 3)
    row = (frames, W, C)
    lift = jnp.asarray(lift_matrices(), BF16)
    parts = []
    for side, (halo, near, far) in enumerate(((above, m0, m1), (below, m3, m2))):
        parts.append(call(functools.partial(stage_two, side), "stage_two_%d" % side,
                          (halo, near, far, mid, coarse, lift, conv_first, conv_second),
                          [(row, BF16), (row, F32), (row, F32)],
                          [pads(6), planes(3), planes(3)], 5))
    out = None
    for side, halo in enumerate((above2, below2)):
        out = last_stage(side, "stage_three_%d" % side, (halo, coarse, lift, *parts[side], conv_first, conv_second,
                                                         parts[1 - side][0]),
                         out, fine.shape[1])
    return out


def solution(mesh):
    split = P("tm", "space", None, None)
    return jax.shard_map(
        local,
        mesh=mesh,
        in_specs=(split, split, P(), P(), P(), P(), P(), P()),
        out_specs=split,
        check_vma=False,
    )
```

```python
import functools

import jax
import jax.numpy as jnp
import numpy as np
from jax import lax
from jax.experimental import pallas as pl
from jax.experimental.pallas import tpu as pltpu
from jax.sharding import PartitionSpec as P


HEADS = 8
C = 256
D = C // HEADS
W = 256
HALF = W // 2
F32 = jnp.float32
BF16 = jnp.bfloat16
VMEM_LIMIT = 20 * 1024 * 1024


def encode_table(frames, width):
    half = width // 2
    inverse = np.exp(-np.log(10000.0) * 2.0 * np.arange(half) / width)
    angles = np.arange(frames)[:, None] * inverse[None, :]
    table = np.concatenate([np.sin(angles), np.cos(angles)], axis=1).astype(np.float32)
    return np.ascontiguousarray(np.broadcast_to(table[:, :, None], (frames, width, 128)))


def flip():
    return (lax.axis_index("space") + 1) % 2


def dot(a, b):
    return jnp.dot(a, b, preferred_element_type=F32)


def normed_row(x_ref, i, row, pos, norm):
    for half in range(W // 128):
        lanes = slice(half * 128, half * 128 + 128)
        h = x_ref[i, row, lanes, :].T.astype(F32) + pos
        center = h - jnp.sum(h, axis=0, keepdims=True) * (1.0 / C)
        spread = jnp.sum(center * center, axis=0, keepdims=True) * (1.0 / C)
        norm[:, lanes] = (center * lax.rsqrt(spread + 1e-05)).astype(BF16)


def own_row(at_row, row, pos_ref, own_ref, wqkv_ref, q_ref, k_ref, v_ref, norm_s):
    frames = own_ref.shape[0]
    base = lax.axis_index("tm") * frames
    for f in range(frames):
        norm = norm_s.at[at_row * frames + f]
        normed_row(own_ref, f, row, pos_ref[base + f], norm)
        y = dot(wqkv_ref[...], norm[...])
        q_ref[at_row, f] = y[:C]
        k_ref[at_row, f] = y[C:2 * C]
        v_ref[at_row, f] = y[2 * C:]


def other_row(n, row, pos_ref, other_ref, wqkv_ref, norm_s, k_s, v_s):
    frames = other_ref.shape[0]
    base = (1 - lax.axis_index("tm")) * frames
    for f in range(frames):
        norm = norm_s.at[n * frames + f]
        normed_row(other_ref, f, row, pos_ref[base + f], norm)
        y = dot(wqkv_ref[C:], norm[...])
        k_s[n, f] = y[:C]
        v_s[n, f] = y[C:]


def scores(n, lanes, q_ref, key_refs):
    frames = q_ref.shape[1]

    def step(d, acc):
        at = pl.ds(pl.multiple_of(d * HEADS, HEADS), HEADS)
        qs = [q_ref[n, a, at, lanes] for a in range(frames)]
        ks = [ref[n, b, at, lanes] for ref in key_refs for b in range(frames)]
        return tuple(total + q * k for total, (q, k) in zip(acc, [(q, k) for q in qs for k in ks]))

    zero = jnp.zeros((HEADS, 128), F32)
    return lax.fori_loop(0, D, step, (zero,) * (frames * frames * len(key_refs)), unroll=16 // len(key_refs))


def attend_row(n, q_ref, ko_ref, vo_ref, k_s, v_s, att_s, prior_ref=None):
    frames = q_ref.shape[1]
    keys = 2 * frames
    factor = float(np.log2(np.e) / np.sqrt(D))
    for half in range(W // 128):
        lanes = slice(half * 128, half * 128 + 128)
        if prior_ref is None:
            acc = scores(n, lanes, q_ref, (ko_ref, k_s))
        else:
            late = scores(n, lanes, q_ref, (k_s,))
            acc = []
            for a in range(frames):
                acc += [prior_ref[n, half, a * frames + b] for b in range(frames)]
                acc += late[a * frames:(a + 1) * frames]
        weights = []
        for a in range(frames):
            line = acc[a * keys:(a + 1) * keys]
            top = line[0]
            for s in line[1:]:
                top = jnp.maximum(top, s)
            powers = [jnp.exp2((s - top) * factor) for s in line]
            total = powers[0]
            for p in powers[1:]:
                total = total + p
            inv = 1.0 / total
            weights += [p * inv for p in powers]

        def gather(d2, _):
            outs = [[] for _ in range(frames)]
            for sub in range(2):
                at = pl.ds(pl.multiple_of(d2 * 2 * HEADS + sub * HEADS, HEADS), HEADS)
                vs = [vo_ref[n, b, at, lanes] for b in range(frames)] + [v_s[n, b, at, lanes] for b in range(frames)]
                for a in range(frames):
                    total = weights[a * keys] * vs[0]
                    for b in range(1, keys):
                        total = total + weights[a * keys + b] * vs[b]
                    outs[a].append(total)
            at = pl.ds(pl.multiple_of(d2 * 2 * HEADS, 2 * HEADS), 2 * HEADS)
            for a in range(frames):
                att_s[n, a, at, lanes] = jnp.concatenate(outs[a], axis=0).astype(BF16)
            return 0

        lax.fori_loop(0, D // 2, gather, 0, unroll=4)


def out_row(n, row, own_ref, wo_ref, att_s, out_ref):
    for a in range(own_ref.shape[0]):
        branch = lax.dot_general(att_s[n, a], wo_ref[...], (((0,), (0,)), ((), ())), preferred_element_type=F32)
        out_ref[a, :W] = (own_ref[a, row].astype(F32) + branch).astype(BF16)


def own_body(pos_hbm, own_hbm, wq_hbm, wk_hbm, wv_hbm, wo_hbm,
             pos_ref, own_ref, wqkv_ref, wor_ref, q_ref, k_ref, v_ref, prior_ref, w_s, norm_s, sems):
    loads = [pltpu.make_async_copy(ref, w_s.at[n], sems.at[n]) for n, ref in enumerate((wq_hbm, wk_hbm, wv_hbm, wo_hbm))]
    loads.append(pltpu.make_async_copy(pos_hbm, pos_ref, sems.at[4]))
    loads.append(pltpu.make_async_copy(own_hbm, own_ref, sems.at[5]))
    for load in loads:
        load.start()
    to = lax.broadcasted_iota(jnp.int32, (C, C), 0)
    at = lax.broadcasted_iota(jnp.int32, (C, C), 1)
    pick = (at == (to % HEADS) * D + to // HEADS).astype(BF16)
    nt = (((1,), (1,)), ((), ()))
    for load in loads[:4]:
        load.wait()
    for n in range(3):
        wqkv_ref[n * C:(n + 1) * C] = lax.dot_general(pick, w_s[n], nt, preferred_element_type=F32).astype(BF16)
    wor_ref[...] = dot(pick, w_s[3]).astype(BF16)
    for load in loads[4:]:
        load.wait()
    start, last = flip() * (own_ref.shape[1] - 1), own_ref.shape[1] - 1
    for n, row in enumerate((start, last - start)):
        own_row(n, row, pos_ref, own_ref, wqkv_ref, q_ref, k_ref, v_ref, norm_s)
    for n in range(2):
        for half in range(W // 128):
            lanes = slice(half * 128, half * 128 + 128)
            for i, total in enumerate(scores(n, lanes, q_ref, (k_ref,))):
                prior_ref[n, half, i] = total


def outer_body(pos_ref, own_ref, other_ref, wqkv_ref, wo_ref, q_ref, k_ref, v_ref, prior_ref,
               down_ref, up_ref, norm_s, k_s, v_s, att_s):
    start, last = flip() * (own_ref.shape[1] - 1), own_ref.shape[1] - 1
    rows = (start, last - start)
    for n, row in enumerate(rows):
        other_row(n, row, pos_ref, other_ref, wqkv_ref, norm_s, k_s, v_s)
    for n in range(2):
        attend_row(n, q_ref, k_ref, v_ref, k_s, v_s, att_s, prior_ref)
    for n, (row, ref) in enumerate(zip(rows, (down_ref, up_ref))):
        out_row(n, row, own_ref, wo_ref, att_s, ref)


def inner_body(pos_ref, own_ref, other_ref, wqkv_ref, wo_ref, coarse_ref, before_ref, down_ref, up_ref,
               norm_s, k_s, v_s, att_s, q_s, ko_s, vo_s, normo_s):
    del before_ref
    start = 1 + flip() * (own_ref.shape[1] - 3)
    rows = (start, own_ref.shape[1] - 1 - start)
    for n, row in enumerate(rows):
        own_row(n, row, pos_ref, own_ref, wqkv_ref, q_s, ko_s, vo_s, normo_s)
        other_row(n, row, pos_ref, other_ref, wqkv_ref, norm_s, k_s, v_s)
    for n in range(2):
        attend_row(n, q_s, ko_s, vo_s, k_s, v_s, att_s)
    for n, (row, ref) in enumerate(zip(rows, (down_ref, up_ref))):
        out_row(n, row, own_ref, wo_ref, att_s, ref)
        ref[:, W:] = coarse_ref[:, flip() ^ n]


def call(body, args, outs, scratch, micros, space=pltpu.VMEM):
    return pl.pallas_call(
        body,
        in_specs=[pl.BlockSpec(memory_space=space)] * len(args),
        out_specs=[pl.BlockSpec(memory_space=pltpu.VMEM)] * len(outs),
        out_shape=[jax.ShapeDtypeStruct(s, t) for s, t in outs],
        scratch_shapes=scratch,
        compiler_params=pltpu.CompilerParams(vmem_limit_bytes=VMEM_LIMIT),
        cost_estimate=pl.CostEstimate(flops=micros * 10**9, transcendentals=0, bytes_accessed=1 << 20),
    )(*args)


def own_projections(pos, own, *weights):
    frames, _ = own.shape[:2]
    wide = ((2, frames, C, W), F32)
    args = [pltpu.with_memory_space_constraint(a, pltpu.HBM) for a in (pos, own, *weights)]
    return call(own_body, args,
                [(pos.shape, F32), (own.shape, BF16), ((3 * C, C), BF16), ((C, C), BF16), wide, wide, wide,
                 ((2, W // 128, frames * frames, HEADS, 128), F32)],
                [pltpu.VMEM((4, C, C), BF16), pltpu.VMEM((2 * frames, C, W), BF16), pltpu.SemaphoreType.DMA((6,))], 6, pltpu.HBM)


def attention(body, args, width, extra, micros):
    frames = args[1].shape[0]
    return call(body, args, [((frames, width, C), BF16)] * 2,
                [pltpu.VMEM((2 * frames, C, W), BF16), pltpu.VMEM((2, frames, C, W), F32),
                 pltpu.VMEM((2, frames, C, W), F32), pltpu.VMEM((2, frames, C, W), BF16)] + extra, micros)


def clear_pads(pad_s):
    for r in range(pad_s.shape[0]):
        pad_s[r, 0:8] = jnp.zeros((8, C), F32)
        pad_s[r, 8 + W:16 + W] = jnp.zeros((8, C), F32)


def shifted(value, pad, out_s, row):
    pad[8:8 + W] = value.astype(F32)
    at = slice(row * W, (row + 1) * W)
    out_s[1, at] = value
    out_s[0, at] = pad[7:7 + W].astype(BF16)
    out_s[2, at] = pad[9:9 + W].astype(BF16)


def taps(source_s, row, w_ref, total=None, steps=(0, 1, 2)):
    turned = flip()
    for n, dy in enumerate(steps):
        tap = dy + turned * (2 - 2 * dy)
        for dx in range(3):
            part = dot(source_s[dx, (row + n) * W:(row + n + 1) * W], w_ref[tap, dx])
            total = part if total is None else total + part
    return total


def relu(value):
    return jnp.maximum(value, jnp.zeros((), value.dtype))


def lift_matrices():
    x, at = np.indices((W, W))
    col = at % HALF
    near = x // 2
    far = np.clip(near + 2 * (x % 2) - 1, 0, HALF - 1)
    base = 0.75 * (col == near) + 0.25 * (col == far)
    second = at // HALF == 1
    return np.stack([base * np.where(second, 0.75, 0.25), base * np.where(second, 0.25, 0.75)]).astype(np.float32)


def stage_one(m0_ref, m1_ref, m2_ref, m3_ref, w1_ref, mid_ref, pad_s, in_s):
    clear_pads(pad_s)

    def frame(f, _):
        for r, ref in enumerate((m0_ref, m1_ref, m2_ref, m3_ref)):
            shifted(relu(ref[f, :W]), pad_s.at[r], in_s, r)
        for j in range(2):
            mid_ref[f, j] = relu(taps(in_s, j, w1_ref)).astype(BF16)
        return 0

    lax.fori_loop(0, m0_ref.shape[0], frame, 0)


def at_edge(side):
    here = lax.axis_index("space")
    end = (flip() ^ side) * (lax.axis_size("space") - 1)
    return here == end


def stage_two(side, halo_ref, near_ref, far_ref, mid_ref, coarse_ref, lift_ref, w1_ref, w2_ref,
              inner_ref, first_ref, second_ref, pad_s, in_s, mid_s):
    steps = (0, 1) if side else (1, 2)
    order = 1 - 2 * side
    near = flip() ^ side
    clear_pads(pad_s)

    def frame(f, _):
        for r, ref in enumerate((halo_ref, near_ref, far_ref)[::order]):
            shifted(relu(ref[f, :W]), pad_s.at[r], in_s, r)
        for j in range(2):
            shifted(mid_ref[f, j], pad_s.at[3 + j], mid_s, j + 1 - side)
        shifted(relu(taps(in_s, 0, w1_ref)).astype(BF16), pad_s.at[5], mid_s, 2 * side)
        first_ref[f] = taps(in_s, side, w1_ref, None, steps)
        total = taps(mid_s, 0, w2_ref, dot(lift_ref[1 - near], coarse_ref[f].reshape(2 * HALF, C)))
        inner_ref[f] = (total + far_ref[f, :W].astype(F32)).astype(BF16)
        second_ref[f] = taps(mid_s, side, w2_ref, near_ref[f, :W].astype(F32), steps)
        return 0

    lax.fori_loop(0, near_ref.shape[0], frame, 0)


def stage_three(*refs):
    halos, coarse_ref, lift_ref, parts, w1_ref, w2_ref = refs[:2], refs[2], refs[3], (refs[4:7], refs[7:10]), refs[10], refs[11]
    out_hbm, pad_s, in_s, mid_s, row_s, coarse_s, sems = refs[12:]
    frames = halos[0].shape[0]
    copies = []
    for side in range(2):
        for f in range(frames):
            n = side * frames + f
            copies.append(pltpu.make_async_copy(parts[side][0].at[f], out_hbm.at[f, 1 + (flip() ^ side)], sems.at[n]))
            copies[-1].start()
    clear_pads(pad_s)
    for side in range(2):
        edge = at_edge(side)
        near = flip() ^ side
        step = (2 * side,)
        for f in range(frames):
            n = side * frames + f
            halo_ref, first_ref, second_ref = halos[side], parts[side][1], parts[side][2]
            shifted(relu(halo_ref[f, :W]), pad_s.at[n], in_s, n)
            own = coarse_ref[f, near]
            coarse_s[n, :HALF] = jnp.where(edge, own, halo_ref[f, W:])
            coarse_s[n, HALF:] = own
            value = relu(taps(in_s, n, w1_ref, first_ref[f], step)).astype(BF16)
            value = jnp.where(edge, jnp.zeros_like(value), value)
            shifted(value, pad_s.at[2 * frames + n], mid_s, n)
            total = second_ref[f] + dot(lift_ref[0], coarse_s[n])
            row_s[n] = taps(mid_s, n, w2_ref, total, step).astype(BF16)
            copies.append(pltpu.make_async_copy(row_s.at[n], out_hbm.at[f, 3 * near], sems.at[2 * frames + n]))
            copies[-1].start()
    for copy in copies:
        copy.wait()


def last_stage(args, rows):
    frames = args[0].shape[0]
    return pl.pallas_call(
        stage_three,
        in_specs=[pl.BlockSpec(memory_space=pltpu.VMEM)] * len(args),
        out_specs=pl.BlockSpec(memory_space=pltpu.HBM),
        out_shape=jax.ShapeDtypeStruct((frames, rows, W, C), BF16),
        scratch_shapes=[pads(4 * frames), planes(2 * frames), planes(2 * frames), pltpu.VMEM((2 * frames, W, C), BF16),
                        pltpu.VMEM((2 * frames, 2 * HALF, C), BF16), pltpu.SemaphoreType.DMA((4 * frames,))],
        compiler_params=pltpu.CompilerParams(vmem_limit_bytes=VMEM_LIMIT),
        cost_estimate=pl.CostEstimate(flops=4 * 10**9, transcendentals=0, bytes_accessed=1 << 20),
        name="stage_three",
    )(*args)


def planes(rows):
    return pltpu.VMEM((3, rows * W, C), BF16)


def pads(rows):
    return pltpu.VMEM((rows, W + 16, C), F32)


def local(fine, coarse, w_query, w_key, w_value, w_out, conv_first, conv_second):
    frames = fine.shape[0]
    size = lax.axis_size("space")
    swaps = []
    for first in (0, 1):
        pairs = [(i, i + 1) for i in range(first, size - 1, 2)]
        swaps.append(pairs + [(j, i) for i, j in pairs])
    other = lax.ppermute(fine, "tm", [(0, 1), (1, 0)])
    pos = jnp.asarray(encode_table(2 * frames, C))
    ready = own_projections(pos, fine, w_query, w_key, w_value, w_out)
    held_pos, held, wqkv, wo, *early = ready
    m0, m3 = attention(outer_body, (held_pos, held, other, wqkv, wo, *early), W,
                       [], 5)
    above, below = [lax.ppermute(m, "space", pairs) for m, pairs in zip((m0, m3), swaps)]
    wide = pltpu.VMEM((2, frames, C, W), F32)
    m1, m2 = attention(inner_body, (held_pos, held, other, wqkv, wo, coarse, m0), W + HALF,
                       [wide] * 3 + [pltpu.VMEM((2 * frames, C, W), BF16)], 7)
    above2 = lax.ppermute(m1, "space", swaps[0])
    below2 = lax.ppermute(m2, "space", swaps[1])
    (mid,) = call(stage_one, (m0, m1, m2, m3, conv_first), [((frames, 2, W, C), BF16)],
                  [pads(4), planes(4)], 3)
    row = (frames, W, C)
    lift = jnp.asarray(lift_matrices(), BF16)
    parts = []
    for side, (halo, near, far) in enumerate(((above, m0, m1), (below, m3, m2))):
        parts.append(call(functools.partial(stage_two, side),
                          (halo, near, far, mid, coarse, lift, conv_first, conv_second),
                          [(row, BF16), (row, F32), (row, F32)],
                          [pads(6), planes(3), planes(3)], 5))
    out = last_stage((above2, below2, coarse, lift, *parts[0], *parts[1], conv_first, conv_second), fine.shape[1])
    return out


def solution(mesh):
    split = P("tm", "space", None, None)
    return jax.shard_map(
        local,
        mesh=mesh,
        in_specs=(split, split, P(), P(), P(), P(), P(), P()),
        out_specs=split,
        check_vma=False,
    )
```
